32 devices in a mesh: slab: 4 (over z), col: 8 (over y, x, core).
Axes of the slice: x: 2, y: 2, z: 4, core: 2. Of those that a mesh axis runs over, the one named last changes fastest.
Arguments:
- field: bfloat16 [2, 64, 256, 1024], P(None, 'slab', 'col'), may hold values from -6 to 6
- fine_plane: int32 [32, 256, 1024], P('slab', 'col'), may hold values from 0 to 15, as said below
- fine_frac: int32 [32, 256, 1024], P('slab', 'col'), may hold values from 0 to 7
- counts: int32 [4, 256, 1024], P('slab', 'col'), may hold values from 1 to 8
Outputs:
- fine_color: float32 [256, 1024], P('col', 'slab')
- fine_depth: float32 [256, 1024], P('col', 'slab')
- coarse_color: float32 [256, 1024], P('col', 'slab')
The draws below stay inside these ranges and needn't reach their ends.
Inputs may be any that keep to these rules, and one draw needn't show every extreme that they name: For each ray and slab the positions 8 * fine_plane + fine_frac are nondecreasing over the 8 slots.
All inputs are finite; a program needn't handle non-finite values.
Results may differ from the reference program's by a relative error of at most 0.0003.
Values may be sent and summed in bfloat16 or wider, within the bound.
No kernel may reach another device: no remote copies, remote signals or barrier semaphores. Data moves between devices by JAX's collectives and lax.ppermute only.
A program may use at most 64 MiB of HBM per device.

```python
import jax
import jax.numpy as jnp
from jax import lax

DEPTH_DEV = 16
U_DEV = 32
V = 1024
FINE = 8
NZ = 64
NU = 256
N_SLAB = 4
N_COL = 8


def fine_positions(key):
    slabs = NZ // DEPTH_DEV
    inner = jax.random.fold_in(key, 1013)
    spots = jax.random.randint(inner, (slabs, FINE, NU, V), 0, DEPTH_DEV * 8, dtype=jnp.int32)
    spots = jnp.sort(spots, axis=1)
    return spots.reshape(slabs * FINE, NU, V)


def draw_fine_plane(key, part):
    return fine_positions(key) // 8


def draw_fine_frac(key, part):
    return fine_positions(key) % 8


def set_ends(entries, stream_key, low, top_value):
    longest = entries.shape.index(max(entries.shape))
    spots = []
    for shift in (0, 1):
        where = [jax.random.randint(jax.random.fold_in(stream_key, axis), (), 0, length) for axis, length in enumerate(entries.shape)]
        where[longest] = (where[longest] + shift) % entries.shape[longest]
        spots.append(tuple(where))
    return entries.at[spots[0]].set(low).at[spots[1]].set(top_value)


def block_scale(rng, dims, cuts, least, largest):
    gain, own = 1.0, jax.random.fold_in(rng, 6)
    for axis_at, blocks in cuts:
        draws = jnp.exp(jax.random.uniform(jax.random.fold_in(own, axis_at), (blocks,), jnp.float32, least / len(cuts), largest / len(cuts)))
        gain = gain * jnp.repeat(draws, dims[axis_at] // blocks).reshape([-1 if axis == axis_at else 1 for axis in range(len(dims))])
    return gain


def bell_draw(stream_key, shape, width, reach, shards=(), kind=jnp.bfloat16):
    factor_of = block_scale(stream_key, shape, shards, -0.22, 0.18) if shards else 1.0
    entries = jax.random.normal(stream_key, shape, jnp.float32) * width * factor_of
    return jnp.minimum(jnp.maximum(entries, -reach), reach).astype(kind)


def setup_inputs(seed: int = 0) -> dict:
    key_list = jax.random.split(jax.random.key(seed), 5)
    return {
        "field": bell_draw(key_list[0], (2, NZ, NU, V), 1.0, 6.0, ((1, 4), (2, 8))),
        "fine_plane": draw_fine_plane(jax.random.fold_in(key_list[4], 71), 0),
        "fine_frac": draw_fine_frac(jax.random.fold_in(key_list[4], 71), 0),
        "counts": set_ends(jax.random.randint(key_list[3], (N_SLAB, NU, V), 1, FINE + 1), jax.random.fold_in(key_list[3], 1), 1, FINE).astype(jnp.int32),
    }


def shade(values):
    density = (2.0 / NZ) * jax.nn.softplus(values[0])
    emission = jax.nn.sigmoid(values[1])
    return density, emission


def exclusive_product(factor):
    totals = jnp.cumprod(factor, axis=0)
    return jnp.concatenate([jnp.ones_like(factor[:1]), totals[:-1]], axis=0)


def render_rows(field_rows, plane_rows, frac_rows, count_rows):
    empty = jnp.zeros((2, 1) + field_rows.shape[2:], jnp.bfloat16)
    volume = jnp.concatenate([field_rows, empty], axis=1)
    lower = volume[:, 7:NZ:8].astype(jnp.float32)
    upper = volume[:, 8:NZ + 1:8].astype(jnp.float32)
    density, emission = shade(0.5 * (lower + upper))
    factor = jnp.exp(-8.0 * density)
    opacity = 1.0 - factor
    coarse = jnp.sum(exclusive_product(factor) * opacity * emission, axis=0)
    slots = plane_rows.shape[0]
    slab_of = (jnp.arange(slots, dtype=jnp.int32) // FINE).astype(jnp.int32)
    start = plane_rows + (slab_of * DEPTH_DEV)[:, None, None]
    index = jnp.broadcast_to(start[None], (2,) + start.shape)
    low = jnp.take_along_axis(volume, index, axis=1).astype(jnp.float32)
    high = jnp.take_along_axis(volume, index + 1, axis=1).astype(jnp.float32)
    weight = frac_rows.astype(jnp.float32) / 8.0
    values = (1.0 - weight) * low + weight * high
    density, emission = shade(values)
    position = (jnp.arange(slots, dtype=jnp.int32) % FINE)[:, None, None]
    live = position < jnp.repeat(count_rows, FINE, axis=0)
    factor = jnp.where(live, jnp.exp(-(DEPTH_DEV / FINE) * density), jnp.float32(1.0))
    opacity = 1.0 - factor
    weighted = exclusive_product(factor) * opacity
    color = jnp.sum(weighted * emission, axis=0)
    depth = jnp.sum(weighted * ((start.astype(jnp.float32) + weight) / NZ), axis=0)
    return jnp.stack([color, depth, coarse])


def reference(field, fine_plane, fine_frac, counts):
    def one_block(block):
        first = (block * U_DEV).astype(jnp.int32)
        return render_rows(
            lax.dynamic_slice_in_dim(field, first, U_DEV, 2),
            lax.dynamic_slice_in_dim(fine_plane, first, U_DEV, 1),
            lax.dynamic_slice_in_dim(fine_frac, first, U_DEV, 1),
            lax.dynamic_slice_in_dim(counts, first, U_DEV, 1))

    blocks = lax.map(one_block, jnp.arange(N_COL, dtype=jnp.int32))
    images = jnp.concatenate([blocks[k] for k in range(N_COL)], axis=1)
    padded = jnp.pad(images, ((0, 0), (1, 1), (0, 0)))
    smooth = 0.25 * padded[:, :-2] + 0.5 * padded[:, 1:-1] + 0.25 * padded[:, 2:]
    return smooth[0], smooth[1], smooth[2]
```

```python
import functools

import jax
import jax.numpy as jnp
from jax import lax
from jax.experimental import pallas as pl
from jax.experimental.pallas import tpu as pltpu
from jax.sharding import PartitionSpec as P

LOG2E = 1.4426950408889634
ROWS = 16
LANES = 128
COLOR, DEEP, FINE, COARSE, COARSE_PASS = range(5)
OCTAVES = 24.0
STEPS = 65534.0 / OCTAVES
WIRE = jnp.int16


def vmem():
    return pl.BlockSpec(memory_space=pltpu.VMEM)


def smem():
    return pl.BlockSpec(memory_space=pltpu.SMEM)


def encode(x):
    if WIRE == jnp.float32:
        return x
    y = jnp.maximum(jnp.log2(x) * STEPS + 65535.5, 0.0)
    return (y.astype(jnp.int32) - 32768).astype(jnp.int16)


def decode(code):
    if WIRE == jnp.float32:
        return code
    y = code.astype(jnp.int32).astype(jnp.float32)
    x = jnp.exp2((y - 32767.0) * (1.0 / STEPS))
    return jnp.where(y > -32767.5, x, 0.0)


def shade(raw0, raw1, power):
    soft = jnp.log2(1.0 + jnp.exp2(raw0 * LOG2E))
    return jnp.exp2(soft * power), 1.0 + jnp.tanh(0.5 * raw1)


def march_rows(field, follow, plane, frac, counts, store, here, cols, base, total_depth):
    depth, slots = field.shape[1], plane.shape[0]
    unit = 8 if 8 * depth <= 256 else 1
    size = (ROWS, LANES)

    def load(ch, z):
        return field[ch, z, here, cols] if z < depth else follow[ch, 0, here, cols]

    live = counts[0, here, cols]
    color = jnp.zeros(size, jnp.float32)
    deep = jnp.zeros(size, jnp.float32)
    passed = jnp.ones(size, jnp.float32)
    for i in range(slots):
        place = plane[i, here, cols] * 8 + frac[i, here, cols]
        k = (place & 15).astype(jnp.float32)
        to_odd = jnp.minimum(k, 16.0 - k) * 0.125
        place = place.astype(jnp.float32)
        spot = (place if unit == 8 else plane[i, here, cols].astype(jnp.float32)).astype(jnp.bfloat16)
        even = [load(ch, 0) for ch in (0, 1)]
        odd = [load(ch, 1) for ch in (0, 1)]
        for z in range(1, depth):
            hit = spot >= jnp.bfloat16(unit * z)
            group = even if z % 2 else odd
            for ch in (0, 1):
                group[ch] = jnp.where(hit, load(ch, z + 1), group[ch])
        values = []
        for ch in (0, 1):
            e, o = even[ch].astype(jnp.float32), odd[ch].astype(jnp.float32)
            values.append(e + to_odd * (o - e))
        factor, emission = shade(*values, -(depth / slots) * (2.0 / total_depth))
        factor = jnp.where(live > i, factor, 1.0)
        weight = passed * (1.0 - factor)
        color = color + weight * emission
        deep = deep + weight * (place + base)
        passed = passed * factor
    store(COLOR, 0.5 * color)
    store(DEEP, deep * (1.0 / (8.0 * total_depth)))
    store(FINE, passed)
    color = jnp.zeros(size, jnp.float32)
    passed = jnp.ones(size, jnp.float32)
    for z in range(7, depth, 8):
        values = [
            0.5 * (load(ch, z).astype(jnp.float32) + load(ch, z + 1).astype(jnp.float32))
            for ch in (0, 1)
        ]
        factor, emission = shade(*values, -8.0 * (2.0 / total_depth))
        color = color + passed * (1.0 - factor) * emission
        passed = passed * factor
    store(COARSE, 0.5 * color)
    store(COARSE_PASS, passed)


def march(field, follow, plane, frac, counts, slab, steps, block_of, width, coded):
    _, depth, rows, _ = field.shape
    slots = plane.shape[0]
    total_depth = depth * lax.axis_size("slab")

    def kernel(slab_ref, field, follow, plane, frac, counts, out):
        base = (slab_ref[0] * (8 * depth)).astype(jnp.float32)

        def step(at, carry):
            r = at // (width // LANES)
            c = at % (width // LANES)
            here = pl.ds(pl.multiple_of(r * ROWS, ROWS), ROWS)
            cols = pl.ds(pl.multiple_of(c * LANES, LANES), LANES)

            def store(what, value):
                out[0, what, here, cols] = encode(value) if coded else value

            march_rows(
                field, follow, plane, frac, counts, store, here, cols, base, total_depth
            )
            return carry

        lax.fori_loop(0, (rows // ROWS) * (width // LANES), step, 0)

    def spec(*lead):
        zeros = (0,) * len(lead)
        return pl.BlockSpec(lead + (rows, width), lambda b, s: zeros + (0, block_of(b, s[0])))

    return pl.pallas_call(
        kernel,
        grid_spec=pltpu.PrefetchScalarGridSpec(
            num_scalar_prefetch=1,
            grid=(steps,),
            in_specs=[spec(2, depth), spec(2, 1), spec(slots), spec(slots), spec(1)],
            out_specs=pl.BlockSpec((1, 5, rows, width), lambda b, s: (b, 0, 0, 0)),
        ),
        out_shape=jax.ShapeDtypeStruct(
            (steps, 5, rows, width), WIRE if coded else jnp.float32
        ),
        compiler_params=pltpu.CompilerParams(vmem_limit_bytes=24 << 20),
        cost_estimate=pl.CostEstimate(
            flops=steps * rows * width * 3000, bytes_accessed=steps * rows * width * 128,
            transcendentals=0,
        ),
        name="march",
    )(slab, field, follow, plane, frac, counts)


def join(mine, got, got_first):
    first = [jnp.where(got_first, g, m) for m, g in zip(mine, got)]
    last = [jnp.where(got_first, m, g) for m, g in zip(mine, got)]
    return [
        first[COLOR] + first[FINE] * last[COLOR],
        first[DEEP] + first[FINE] * last[DEEP],
        first[FINE] * last[FINE],
        first[COARSE] + first[COARSE_PASS] * last[COARSE],
        first[COARSE_PASS] * last[COARSE_PASS],
    ]


def halve(mine, got, slab, bit):
    blocks, kinds, rows, width = mine.shape

    def kernel(slab_ref, mine, got, send, keep):
        got_first = (slab_ref[0] >> bit) & 1 == 1
        want = (slab_ref[0] >> (bit + 1)) & 1
        for i in range(blocks // 2):
            for out, at in ((send, 2 * i + 1 - want), (keep, 2 * i + want)):
                for r in range(0, rows, ROWS):
                    here = pl.ds(r, ROWS)
                    done = join(
                        [mine[at, what, here, :] for what in range(kinds)],
                        [decode(got[at, what, here, :]) for what in range(kinds)],
                        got_first,
                    )
                    for what in range(kinds):
                        out[i, what, here, :] = (
                            encode(done[what]) if out is send else done[what]
                        )

    shape = (blocks // 2, kinds, rows, width)
    return pl.pallas_call(
        kernel,
        in_specs=[smem(), vmem(), vmem()],
        out_specs=[vmem(), vmem()],
        out_shape=[jax.ShapeDtypeStruct(shape, WIRE), jax.ShapeDtypeStruct(shape, jnp.float32)],
        compiler_params=pltpu.CompilerParams(vmem_limit_bytes=16 << 20),
        name="halve",
    )(slab, mine, got)


def finish(mine, got, slab, bit, col):
    _, kinds, rows, width = mine.shape
    runs = [mine] if got is None else [mine, got]

    def kernel(slab_ref, col_ref, mine, *refs):
        *partner, image, near, far = refs
        odd = col_ref[0] % 2 == 1
        done = [mine[0, what] for what in range(kinds)]
        for got in partner:
            got_first = (slab_ref[0] >> bit) & 1 == 1
            done = join(done, [decode(got[0, what]) for what in range(kinds)], got_first)
        row = lax.broadcasted_iota(jnp.int32, (rows, width), 0)
        for at, what in enumerate((COLOR, DEEP, COARSE)):
            x = done[what]
            up = jnp.where(row == 0, 0.0, pltpu.roll(x, 1, 0))
            down = jnp.where(row == rows - 1, 0.0, pltpu.roll(x, rows - 1, 0))
            image[at] = 0.25 * up + 0.5 * x + 0.25 * down
            top, bottom = x[0:1], x[rows - 1 : rows]
            near[pl.ds(at, 1), :] = 0.25 * jnp.where(odd, top, bottom)
            far[pl.ds(at, 1), :] = 0.25 * jnp.where(odd, bottom, top)

    edge = jax.ShapeDtypeStruct((3, width), jnp.float32)
    return pl.pallas_call(
        kernel,
        in_specs=[smem(), smem()] + [vmem()] * len(runs),
        out_specs=[vmem()] * 3,
        out_shape=[jax.ShapeDtypeStruct((3, rows, width), jnp.float32), edge, edge],
        compiler_params=pltpu.CompilerParams(vmem_limit_bytes=16 << 20),
        name="finish",
    )(slab, col, *runs)


def border(image, near, far, col):
    _, rows, width = image.shape

    def kernel(col_ref, image, near, far, *outs):
        odd = col_ref[0] % 2 == 1
        row = lax.broadcasted_iota(jnp.int32, (rows, width), 0)
        for at, out in enumerate(outs):
            a, b = near[pl.ds(at, 1), :], far[pl.ds(at, 1), :]
            above, below = jnp.where(odd, a, b), jnp.where(odd, b, a)
            extra = jnp.where(row == 0, above, 0.0) + jnp.where(row == rows - 1, below, 0.0)
            out[...] = image[at] + extra

    return pl.pallas_call(
        kernel,
        in_specs=[smem()] + [vmem()] * 3,
        out_specs=[vmem()] * 3,
        out_shape=[jax.ShapeDtypeStruct((rows, width), jnp.float32)] * 3,
        compiler_params=pltpu.CompilerParams(vmem_limit_bytes=16 << 20),
        name="border",
    )(col, image, near, far)


def pairs(low, high):
    route = list(zip(low, high))
    return route + [(b, a) for a, b in route]


def neighbours(near, far):
    count = lax.axis_size("col")
    near = lax.ppermute(near, "col", pairs(range(0, count - 1, 2), range(1, count, 2)))
    far = lax.ppermute(far, "col", pairs(range(1, count - 1, 2), range(2, count, 2)))
    return near, far


def wide_exchange(parts, slabs, width):
    blocks, kinds, rows, lanes = parts.shape
    tiles = parts.transpose(1, 2, 0, 3).reshape(kinds, rows, slabs, width).transpose(2, 0, 1, 3)
    got = lax.all_to_all(tiles, "slab", 0, 0)
    done = [got[0, what] for what in range(kinds)]
    for s in range(1, slabs):
        done = join(done, [got[s, what] for what in range(kinds)], False)
    return jnp.stack(done)[None]


def body(field, fine_plane, fine_frac, counts):
    slabs = lax.axis_size("slab")
    columns = field.shape[3]
    width = columns // slabs
    slab = lax.axis_index("slab").reshape(1).astype(jnp.int32)
    col = lax.axis_index("col").reshape(1).astype(jnp.int32)
    follow = lax.ppermute(field[:, :1], "slab", [(i + 1, i) for i in range(slabs - 1)])
    args = (field, follow, fine_plane, fine_frac, counts, slab)
    if width % LANES:
        parts = march(*args, columns // LANES, lambda b, s: b, LANES, False)
        image, near, far = finish(wide_exchange(parts, slabs, width), None, slab, 0, col)
        return border(image, *neighbours(near, far), col)
    send = march(*args, slabs // 2, lambda b, s: 2 * b + 1 - (s & 1), width, True)
    keep = march(*args, slabs // 2, lambda b, s: 2 * b + (s & 1), width, False)
    bit = 0
    while True:
        low = [i for i in range(slabs) if not (i >> bit) & 1]
        got = lax.ppermute(send, "slab", pairs(low, [i + (1 << bit) for i in low]))
        if 2 << bit == slabs:
            break
        send, keep = halve(keep, got, slab, bit)
        bit += 1
    image, near, far = finish(keep, got, slab, bit, col)
    near, far = neighbours(near, far)
    return border(image, near, far, col)


def solution(mesh):
    in_specs = (
        P(None, "slab", "col", None),
        P("slab", "col", None),
        P("slab", "col", None),
        P("slab", "col", None),
    )
    out_specs = (P("col", "slab"), P("col", "slab"), P("col", "slab"))
    return jax.shard_map(body, mesh=mesh, in_specs=in_specs, out_specs=out_specs, check_vma=False)
```

```python
import functools

import jax
import jax.numpy as jnp
from jax import lax
from jax.experimental import pallas as pl
from jax.experimental.pallas import tpu as pltpu
from jax.sharding import PartitionSpec as P

LOG2E = 1.4426950408889634
ROWS = 16
LANES = 128
COLOR, DEEP, FINE, COARSE, COARSE_PASS = range(5)
OCTAVES = 24.0
STEPS = 65534.0 / OCTAVES
WIRE = jnp.int16
MARCH_LIMIT = 24 << 20


def vmem():
    return pl.BlockSpec(memory_space=pltpu.VMEM)


def smem():
    return pl.BlockSpec(memory_space=pltpu.SMEM)


def encode(x):
    if WIRE == jnp.float32:
        return x
    y = jnp.maximum(jnp.log2(x) * STEPS + 65535.5, 0.0)
    return (y.astype(jnp.int32) - 32768).astype(jnp.int16)


def decode(code):
    if WIRE == jnp.float32:
        return code
    y = code.astype(jnp.int32).astype(jnp.float32)
    x = jnp.exp2((y - 32767.0) * (1.0 / STEPS))
    return jnp.where(y > -32767.5, x, 0.0)


def shade(raw0, raw1, power):
    soft = jnp.log2(1.0 + jnp.exp2(raw0 * LOG2E))
    return jnp.exp2(soft * power), 1.0 + jnp.tanh(0.5 * raw1)


def march_rows(field, plane, frac, counts, run, late, here, cols, base, total_depth):
    depth, slots = field.shape[1], plane.shape[0]
    unit = 8 if 8 * depth <= 256 else 1
    size = (ROWS, LANES)
    live = counts[0, here, cols]
    color = jnp.zeros(size, jnp.float32)
    deep = jnp.zeros(size, jnp.float32)
    passed = jnp.ones(size, jnp.float32)
    for i in range(slots):
        place = plane[i, here, cols] * 8 + frac[i, here, cols]
        k = (place & 15).astype(jnp.float32)
        to_odd = jnp.minimum(k, 16.0 - k) * 0.125
        place = place.astype(jnp.float32)
        spot = place if unit == 8 else plane[i, here, cols].astype(jnp.float32)
        spot = spot.astype(jnp.bfloat16)
        even = [field[ch, 0, here, cols] for ch in (0, 1)]
        odd = [field[ch, 1, here, cols] for ch in (0, 1)]
        for z in range(1, depth - 1):
            hit = spot >= jnp.bfloat16(unit * z)
            group = even if z % 2 else odd
            for ch in (0, 1):
                group[ch] = jnp.where(hit, field[ch, z + 1, here, cols], group[ch])
        values = []
        for ch in (0, 1):
            e, o = even[ch].astype(jnp.float32), odd[ch].astype(jnp.float32)
            values.append(e + to_odd * (o - e))
        factor, emission = shade(*values, -(depth / slots) * (2.0 / total_depth))
        rest = jnp.where(live > i, place - 8.0 * (depth - 1), -1.0)
        early = (live > i) & (place < 8.0 * (depth - 1))
        late[i, here, cols] = jnp.maximum(rest, -1.0).astype(jnp.bfloat16)
        factor = jnp.where(early, factor, 1.0)
        weight = passed * (1.0 - factor)
        color = color + weight * emission
        deep = deep + weight * (place + base)
        passed = passed * factor
    run[COLOR, here, cols] = color
    run[DEEP, here, cols] = deep
    run[FINE, here, cols] = passed
    color = jnp.zeros(size, jnp.float32)
    passed = jnp.ones(size, jnp.float32)
    for z in range(7, depth - 1, 8):
        values = [
            0.5 * (field[ch, z, here, cols].astype(jnp.float32)
                   + field[ch, z + 1, here, cols].astype(jnp.float32))
            for ch in (0, 1)
        ]
        factor, emission = shade(*values, -8.0 * (2.0 / total_depth))
        color = color + passed * (1.0 - factor) * emission
        passed = passed * factor
    run[COARSE, here, cols] = color
    run[COARSE_PASS, here, cols] = passed


def tiles(rows, width, step):
    across = width // LANES

    def one(at, carry):
        here = pl.ds(pl.multiple_of((at // across) * ROWS, ROWS), ROWS)
        step(here, pl.ds(pl.multiple_of((at % across) * LANES, LANES), LANES))
        return carry

    lax.fori_loop(0, (rows // ROWS) * across, one, 0)


def march(field, plane, frac, counts, slab, width):
    _, depth, rows, columns = field.shape
    slots, blocks = plane.shape[0], columns // width
    total_depth = depth * lax.axis_size("slab")

    def kernel(slab_ref, field, plane, frac, counts, run, late, last):
        base = (slab_ref[0] * (8 * depth)).astype(jnp.float32)
        last[0] = field[:, depth - 1]
        tiles(rows, width, lambda here, cols: march_rows(
            field, plane, frac, counts, run.at[0], late.at[0], here, cols, base, total_depth
        ))

    def spec(*lead):
        zeros = (0,) * len(lead)
        return pl.BlockSpec(lead + (rows, width), lambda b: zeros + (0, b))

    def out(*lead):
        zeros = (0,) * len(lead)
        return pl.BlockSpec((1,) + lead + (rows, width), lambda b: (b,) + zeros + (0, 0))

    def shape(*lead, kind):
        return jax.ShapeDtypeStruct((blocks,) + lead + (rows, width), kind)

    return pl.pallas_call(
        kernel,
        grid=(blocks,),
        in_specs=[smem(), spec(2, depth), spec(slots), spec(slots), spec(1)],
        out_specs=[out(5), out(slots), out(2)],
        out_shape=[
            shape(5, kind=jnp.float32), shape(slots, kind=jnp.bfloat16),
            shape(2, kind=jnp.bfloat16),
        ],
        compiler_params=pltpu.CompilerParams(vmem_limit_bytes=MARCH_LIMIT),
        cost_estimate=pl.CostEstimate(
            flops=rows * columns * 3000, bytes_accessed=rows * columns * 128, transcendentals=0
        ),
        name="march",
    )(slab, *(pltpu.with_memory_space_constraint(x, pltpu.HBM) for x in (field, plane, frac, counts)))


def close(run, late, last, follow, slab, depth, steps, block_of, coded):
    _, slots, rows, width = late.shape
    total_depth = depth * lax.axis_size("slab")

    def kernel(slab_ref, run, late, last, follow, out):
        s = slab_ref[0]
        base = (s * (8 * depth) + 8 * (depth - 1)).astype(jnp.float32)

        def step(i, here, cols):
            b = block_of(i, s)
            there = pl.ds(pl.multiple_of(b * width + cols.start, LANES), LANES)
            low = [last[b, ch, here, cols].astype(jnp.float32) for ch in (0, 1)]
            high = [follow[ch, 0, here, there].astype(jnp.float32) for ch in (0, 1)]
            slope = [(h - l) * 0.125 for h, l in zip(high, low)]
            color, deep, passed = (run[b, what, here, cols] for what in (COLOR, DEEP, FINE))
            for k in range(slots):
                eighths = late[b, k, here, cols].astype(jnp.float32)
                values = [l + eighths * d for l, d in zip(low, slope)]
                factor, emission = shade(*values, -(depth / slots) * (2.0 / total_depth))
                factor = jnp.where(eighths >= 0.0, factor, 1.0)
                weight = passed * (1.0 - factor)
                color = color + weight * emission
                deep = deep + weight * (eighths + base)
                passed = passed * factor
            values = [0.5 * (h + l) for h, l in zip(high, low)]
            factor, emission = shade(*values, -8.0 * (2.0 / total_depth))
            coarse, through = (run[b, what, here, cols] for what in (COARSE, COARSE_PASS))
            coarse = coarse + through * (1.0 - factor) * emission
            done = {
                COLOR: 0.5 * color, DEEP: deep * (1.0 / (8.0 * total_depth)), FINE: passed,
                COARSE: 0.5 * coarse, COARSE_PASS: through * factor,
            }
            for what, value in done.items():
                out[i, what, here, cols] = encode(value) if coded else value

        for i in range(steps):
            tiles(rows, width, functools.partial(step, i))

    return pl.pallas_call(
        kernel,
        in_specs=[smem()] + [vmem()] * 4,
        out_specs=vmem(),
        out_shape=jax.ShapeDtypeStruct((steps, 5, rows, width), WIRE if coded else jnp.float32),
        compiler_params=pltpu.CompilerParams(vmem_limit_bytes=24 << 20),
        cost_estimate=pl.CostEstimate(
            flops=steps * rows * width * 1500, bytes_accessed=steps * rows * width * 64,
            transcendentals=0,
        ),
        name="close",
    )(slab, run, late, last, follow)


def join(mine, got, got_first):
    first = [jnp.where(got_first, g, m) for m, g in zip(mine, got)]
    last = [jnp.where(got_first, m, g) for m, g in zip(mine, got)]
    return [
        first[COLOR] + first[FINE] * last[COLOR],
        first[DEEP] + first[FINE] * last[DEEP],
        first[FINE] * last[FINE],
        first[COARSE] + first[COARSE_PASS] * last[COARSE],
        first[COARSE_PASS] * last[COARSE_PASS],
    ]


def halve(mine, got, slab, bit):
    blocks, kinds, rows, width = mine.shape

    def kernel(slab_ref, mine, got, send, keep):
        got_first = (slab_ref[0] >> bit) & 1 == 1
        want = (slab_ref[0] >> (bit + 1)) & 1
        for i in range(blocks // 2):
            for out, at in ((send, 2 * i + 1 - want), (keep, 2 * i + want)):
                for r in range(0, rows, ROWS):
                    here = pl.ds(r, ROWS)
                    done = join(
                        [mine[at, what, here, :] for what in range(kinds)],
                        [decode(got[at, what, here, :]) for what in range(kinds)],
                        got_first,
                    )
                    for what in range(kinds):
                        out[i, what, here, :] = (
                            encode(done[what]) if out is send else done[what]
                        )

    shape = (blocks // 2, kinds, rows, width)
    return pl.pallas_call(
        kernel,
        in_specs=[smem(), vmem(), vmem()],
        out_specs=[vmem(), vmem()],
        out_shape=[jax.ShapeDtypeStruct(shape, WIRE), jax.ShapeDtypeStruct(shape, jnp.float32)],
        compiler_params=pltpu.CompilerParams(vmem_limit_bytes=16 << 20),
        name="halve",
    )(slab, mine, got)


def finish(mine, got, slab, bit, col):
    _, kinds, rows, width = mine.shape
    runs = [mine] if got is None else [mine, got]

    def kernel(slab_ref, col_ref, mine, *refs):
        *partner, image, near, far = refs
        odd = col_ref[0] % 2 == 1
        done = [mine[0, what] for what in range(kinds)]
        for got in partner:
            got_first = (slab_ref[0] >> bit) & 1 == 1
            done = join(done, [decode(got[0, what]) for what in range(kinds)], got_first)
        row = lax.broadcasted_iota(jnp.int32, (rows, width), 0)
        for at, what in enumerate((COLOR, DEEP, COARSE)):
            x = done[what]
            up = jnp.where(row == 0, 0.0, pltpu.roll(x, 1, 0))
            down = jnp.where(row == rows - 1, 0.0, pltpu.roll(x, rows - 1, 0))
            image[at] = 0.25 * up + 0.5 * x + 0.25 * down
            top, bottom = x[0:1], x[rows - 1 : rows]
            near[pl.ds(at, 1), :] = 0.25 * jnp.where(odd, top, bottom)
            far[pl.ds(at, 1), :] = 0.25 * jnp.where(odd, bottom, top)

    edge = jax.ShapeDtypeStruct((3, width), jnp.float32)
    return pl.pallas_call(
        kernel,
        in_specs=[smem(), smem()] + [vmem()] * len(runs),
        out_specs=[vmem()] * 3,
        out_shape=[jax.ShapeDtypeStruct((3, rows, width), jnp.float32), edge, edge],
        compiler_params=pltpu.CompilerParams(vmem_limit_bytes=16 << 20),
        name="finish",
    )(slab, col, *runs)


def border(image, near, far, col):
    _, rows, width = image.shape

    def kernel(col_ref, image, near, far, *outs):
        odd = col_ref[0] % 2 == 1
        row = lax.broadcasted_iota(jnp.int32, (rows, width), 0)
        for at, out in enumerate(outs):
            a, b = near[pl.ds(at, 1), :], far[pl.ds(at, 1), :]
            above, below = jnp.where(odd, a, b), jnp.where(odd, b, a)
            extra = jnp.where(row == 0, above, 0.0) + jnp.where(row == rows - 1, below, 0.0)
            out[...] = image[at] + extra

    return pl.pallas_call(
        kernel,
        in_specs=[smem()] + [vmem()] * 3,
        out_specs=[vmem()] * 3,
        out_shape=[jax.ShapeDtypeStruct((rows, width), jnp.float32)] * 3,
        compiler_params=pltpu.CompilerParams(vmem_limit_bytes=16 << 20),
        name="border",
    )(col, image, near, far)


def pairs(low, high):
    route = list(zip(low, high))
    return route + [(b, a) for a, b in route]


def neighbours(near, far):
    count = lax.axis_size("col")
    far = lax.ppermute(far, "col", pairs(range(1, count - 1, 2), range(2, count, 2)))
    near = lax.ppermute(near, "col", pairs(range(0, count - 1, 2), range(1, count, 2)))
    return near, far


def wide_exchange(parts, slabs, width):
    blocks, kinds, rows, lanes = parts.shape
    tiles = parts.transpose(1, 2, 0, 3).reshape(kinds, rows, slabs, width).transpose(2, 0, 1, 3)
    got = lax.all_to_all(tiles, "slab", 0, 0)
    done = [got[0, what] for what in range(kinds)]
    for s in range(1, slabs):
        done = join(done, [got[s, what] for what in range(kinds)], False)
    return jnp.stack(done)[None]


def body(field, fine_plane, fine_frac, counts):
    slabs = lax.axis_size("slab")
    columns = field.shape[3]
    width = columns // slabs
    slab = lax.axis_index("slab").reshape(1).astype(jnp.int32)
    col = lax.axis_index("col").reshape(1).astype(jnp.int32)
    follow = lax.ppermute(field[:, :1], "slab", [(i + 1, i) for i in range(slabs - 1)])
    block = width if width % LANES == 0 else LANES
    ahead = march(field, fine_plane, fine_frac, counts, slab, block)
    close_ = functools.partial(close, *ahead, follow, slab, field.shape[1])
    if width != block:
        parts = close_(columns // block, lambda b, s: b, False)
        image, near, far = finish(wide_exchange(parts, slabs, width), None, slab, 0, col)
        return border(image, *neighbours(near, far), col)
    send = close_(slabs // 2, lambda b, s: 2 * b + 1 - (s & 1), True)
    keep = close_(slabs // 2, lambda b, s: 2 * b + (s & 1), False)
    bit = 0
    while True:
        low = [i for i in range(slabs) if not (i >> bit) & 1]
        got = lax.ppermute(send, "slab", pairs(low, [i + (1 << bit) for i in low]))
        if 2 << bit == slabs:
            break
        send, keep = halve(keep, got, slab, bit)
        bit += 1
    image, near, far = finish(keep, got, slab, bit, col)
    near, far = neighbours(near, far)
    return border(image, near, far, col)


def solution(mesh):
    in_specs = (
        P(None, "slab", "col", None),
        P("slab", "col", None),
        P("slab", "col", None),
        P("slab", "col", None),
    )
    out_specs = (P("col", "slab"), P("col", "slab"), P("col", "slab"))
    return jax.shard_map(body, mesh=mesh, in_specs=in_specs, out_specs=out_specs, check_vma=False)
```

```python
import functools

import jax
import jax.numpy as jnp
from jax import lax
from jax.experimental import pallas as pl
from jax.experimental.pallas import tpu as pltpu
from jax.sharding import PartitionSpec as P

LOG2E = 1.4426950408889634
ROWS = 16
LANES = 128
COLOR, DEEP, FINE, COARSE, COARSE_PASS = range(5)
OCTAVES = 24.0
STEPS = 65534.0 / OCTAVES
WIRE = jnp.int16


def vmem():
    return pl.BlockSpec(memory_space=pltpu.VMEM)


def smem():
    return pl.BlockSpec(memory_space=pltpu.SMEM)


def encode(x):
    if WIRE == jnp.float32:
        return x
    y = jnp.maximum(jnp.log2(x) * STEPS + 65535.5, 0.0)
    return (y.astype(jnp.int32) - 32768).astype(jnp.int16)


def decode(code):
    if WIRE == jnp.float32:
        return code
    y = code.astype(jnp.int32).astype(jnp.float32)
    x = jnp.exp2((y - 32767.0) * (1.0 / STEPS))
    return jnp.where(y > -32767.5, x, 0.0)


def shade(raw0, raw1, power):
    soft = jnp.log2(1.0 + jnp.exp2(raw0 * LOG2E))
    return jnp.exp2(soft * power), 1.0 + jnp.tanh(0.5 * raw1)


def march_rows(field, plane, frac, counts, run, late, here, cols, base, total_depth):
    depth, slots = field.shape[1], plane.shape[0]
    unit = 8 if 8 * depth <= 256 else 1
    size = (ROWS, LANES)
    live = counts[0, here, cols]
    color = jnp.zeros(size, jnp.float32)
    deep = jnp.zeros(size, jnp.float32)
    passed = jnp.ones(size, jnp.float32)
    for i in range(slots):
        place = plane[i, here, cols] * 8 + frac[i, here, cols]
        k = (place & 15).astype(jnp.float32)
        to_odd = jnp.minimum(k, 16.0 - k) * 0.125
        place = place.astype(jnp.float32)
        spot = place if unit == 8 else plane[i, here, cols].astype(jnp.float32)
        spot = spot.astype(jnp.bfloat16)
        even = [field[ch, 0, here, cols] for ch in (0, 1)]
        odd = [field[ch, 1, here, cols] for ch in (0, 1)]
        for z in range(1, depth - 1):
            hit = spot >= jnp.bfloat16(unit * z)
            group = even if z % 2 else odd
            for ch in (0, 1):
                group[ch] = jnp.where(hit, field[ch, z + 1, here, cols], group[ch])
        values = []
        for ch in (0, 1):
            e, o = even[ch].astype(jnp.float32), odd[ch].astype(jnp.float32)
            values.append(e + to_odd * (o - e))
        factor, emission = shade(*values, -(depth / slots) * (2.0 / total_depth))
        rest = jnp.where(live > i, place - 8.0 * (depth - 1), -1.0)
        early = (live > i) & (place < 8.0 * (depth - 1))
        late[i, here, cols] = jnp.maximum(rest, -1.0).astype(jnp.bfloat16)
        factor = jnp.where(early, factor, 1.0)
        weight = passed * (1.0 - factor)
        color = color + weight * emission
        deep = deep + weight * (place + base)
        passed = passed * factor
    run[COLOR, here, cols] = color
    run[DEEP, here, cols] = deep
    run[FINE, here, cols] = passed
    color = jnp.zeros(size, jnp.float32)
    passed = jnp.ones(size, jnp.float32)
    for z in range(7, depth - 1, 8):
        values = [
            0.5 * (field[ch, z, here, cols].astype(jnp.float32)
                   + field[ch, z + 1, here, cols].astype(jnp.float32))
            for ch in (0, 1)
        ]
        factor, emission = shade(*values, -8.0 * (2.0 / total_depth))
        color = color + passed * (1.0 - factor) * emission
        passed = passed * factor
    run[COARSE, here, cols] = color
    run[COARSE_PASS, here, cols] = passed


def tiles(rows, width, step):
    across = width // LANES

    def one(at, carry):
        here = pl.ds(pl.multiple_of((at // across) * ROWS, ROWS), ROWS)
        step(here, pl.ds(pl.multiple_of((at % across) * LANES, LANES), LANES))
        return carry

    lax.fori_loop(0, (rows // ROWS) * across, one, 0)


def march(field, plane, frac, counts, slab, steps, block_of, width):
    _, depth, rows, _ = field.shape
    slots = plane.shape[0]
    total_depth = depth * lax.axis_size("slab")

    def kernel(slab_ref, field, plane, frac, counts, run, late, last):
        base = (slab_ref[0] * (8 * depth)).astype(jnp.float32)
        last[0] = field[:, depth - 1]
        tiles(rows, width, lambda here, cols: march_rows(
            field, plane, frac, counts, run.at[0], late.at[0], here, cols, base, total_depth
        ))

    def spec(*lead):
        zeros = (0,) * len(lead)
        return pl.BlockSpec(lead + (rows, width), lambda b, s: zeros + (0, block_of(b, s[0])))

    def out(*lead):
        zeros = (0,) * len(lead)
        return pl.BlockSpec((1,) + lead + (rows, width), lambda b, s: (b,) + zeros + (0, 0))

    def shape(*lead, kind):
        return jax.ShapeDtypeStruct((steps,) + lead + (rows, width), kind)

    return pl.pallas_call(
        kernel,
        grid_spec=pltpu.PrefetchScalarGridSpec(
            num_scalar_prefetch=1,
            grid=(steps,),
            in_specs=[spec(2, depth), spec(slots), spec(slots), spec(1)],
            out_specs=[out(5), out(slots), out(2)],
        ),
        out_shape=[
            shape(5, kind=jnp.float32), shape(slots, kind=jnp.bfloat16),
            shape(2, kind=jnp.bfloat16),
        ],
        compiler_params=pltpu.CompilerParams(vmem_limit_bytes=24 << 20),
        cost_estimate=pl.CostEstimate(
            flops=steps * rows * width * 3000, bytes_accessed=steps * rows * width * 128,
            transcendentals=0,
        ),
        name="march",
    )(slab, *(pltpu.with_memory_space_constraint(x, pltpu.HBM)
              for x in (field, plane, frac, counts)))


def close(ahead, follow, slab, depth, first, steps, block_of, coded):
    run, late, last = ahead
    _, slots, rows, width = late.shape
    total_depth = depth * lax.axis_size("slab")

    def kernel(slab_ref, run, late, last, follow, out):
        s = slab_ref[0]
        base = (s * (8 * depth) + 8 * (depth - 1)).astype(jnp.float32)

        def step(i, here, cols):
            b = first + i
            start = block_of(b, s) * width + cols.start
            there = pl.ds(pl.multiple_of(start, LANES), LANES)
            low = [last[b, ch, here, cols].astype(jnp.float32) for ch in (0, 1)]
            high = [follow[ch, 0, here, there].astype(jnp.float32) for ch in (0, 1)]
            slope = [(h - l) * 0.125 for h, l in zip(high, low)]
            color, deep, passed = (run[b, what, here, cols] for what in (COLOR, DEEP, FINE))
            for k in range(slots):
                eighths = late[b, k, here, cols].astype(jnp.float32)
                values = [l + eighths * d for l, d in zip(low, slope)]
                factor, emission = shade(*values, -(depth / slots) * (2.0 / total_depth))
                factor = jnp.where(eighths >= 0.0, factor, 1.0)
                weight = passed * (1.0 - factor)
                color = color + weight * emission
                deep = deep + weight * (eighths + base)
                passed = passed * factor
            values = [0.5 * (h + l) for h, l in zip(high, low)]
            factor, emission = shade(*values, -8.0 * (2.0 / total_depth))
            coarse, through = (run[b, what, here, cols] for what in (COARSE, COARSE_PASS))
            coarse = coarse + through * (1.0 - factor) * emission
            done = {
                COLOR: 0.5 * color, DEEP: deep * (1.0 / (8.0 * total_depth)), FINE: passed,
                COARSE: 0.5 * coarse, COARSE_PASS: through * factor,
            }
            for what, value in done.items():
                out[i, what, here, cols] = encode(value) if coded else value

        for i in range(steps):
            tiles(rows, width, functools.partial(step, i))

    return pl.pallas_call(
        kernel,
        in_specs=[smem()] + [vmem()] * 4,
        out_specs=vmem(),
        out_shape=jax.ShapeDtypeStruct((steps, 5, rows, width), WIRE if coded else jnp.float32),
        compiler_params=pltpu.CompilerParams(vmem_limit_bytes=24 << 20),
        cost_estimate=pl.CostEstimate(
            flops=steps * rows * width * 1500, bytes_accessed=steps * rows * width * 64,
            transcendentals=0,
        ),
        name="close",
    )(slab, run, late, last, follow)


def join(mine, got, got_first):
    first = [jnp.where(got_first, g, m) for m, g in zip(mine, got)]
    last = [jnp.where(got_first, m, g) for m, g in zip(mine, got)]
    return [
        first[COLOR] + first[FINE] * last[COLOR],
        first[DEEP] + first[FINE] * last[DEEP],
        first[FINE] * last[FINE],
        first[COARSE] + first[COARSE_PASS] * last[COARSE],
        first[COARSE_PASS] * last[COARSE_PASS],
    ]


def relay(mine, got, slab):
    _, kinds, rows, _ = mine.shape

    def kernel(slab_ref, mine, got, send):
        got_first = slab_ref[0] & 1 == 1
        for r in range(0, rows, ROWS):
            here = pl.ds(r, ROWS)
            done = join(
                [mine[0, what, here, :] for what in range(kinds)],
                [decode(got[0, what, here, :]) for what in range(kinds)],
                got_first,
            )
            for what in range(kinds):
                send[0, what, here, :] = encode(done[what])

    return pl.pallas_call(
        kernel,
        in_specs=[smem(), vmem(), vmem()],
        out_specs=vmem(),
        out_shape=jax.ShapeDtypeStruct(got.shape, WIRE),
        compiler_params=pltpu.CompilerParams(vmem_limit_bytes=16 << 20),
        name="relay",
    )(slab, mine, got)


def finish(mine, got, slab, col):
    _, kinds, rows, width = mine.shape
    runs = [mine, *got]

    def kernel(slab_ref, col_ref, mine, *refs):
        *partner, image, near, far = refs
        odd = col_ref[0] % 2 == 1
        done = [mine[0, what] for what in range(kinds)]
        for bit, got in enumerate(partner):
            got_first = (slab_ref[0] >> bit) & 1 == 1
            done = join(done, [decode(got[0, what]) for what in range(kinds)], got_first)
        row = lax.broadcasted_iota(jnp.int32, (rows, width), 0)
        for at, what in enumerate((COLOR, DEEP, COARSE)):
            x = done[what]
            up = jnp.where(row == 0, 0.0, pltpu.roll(x, 1, 0))
            down = jnp.where(row == rows - 1, 0.0, pltpu.roll(x, rows - 1, 0))
            image[at] = 0.25 * up + 0.5 * x + 0.25 * down
            top, bottom = x[0:1], x[rows - 1 : rows]
            near[pl.ds(at, 1), :] = 0.25 * jnp.where(odd, top, bottom)
            far[pl.ds(at, 1), :] = 0.25 * jnp.where(odd, bottom, top)

    edge = jax.ShapeDtypeStruct((3, width), jnp.float32)
    return pl.pallas_call(
        kernel,
        in_specs=[smem(), smem()] + [vmem()] * len(runs),
        out_specs=[vmem()] * 3,
        out_shape=[jax.ShapeDtypeStruct((3, rows, width), jnp.float32), edge, edge],
        compiler_params=pltpu.CompilerParams(vmem_limit_bytes=16 << 20),
        name="finish",
    )(slab, col, *runs)


def border(image, near, far, col):
    _, rows, width = image.shape

    def kernel(col_ref, image, near, far, *outs):
        odd = col_ref[0] % 2 == 1
        row = lax.broadcasted_iota(jnp.int32, (rows, width), 0)
        for at, out in enumerate(outs):
            a, b = near[pl.ds(at, 1), :], far[pl.ds(at, 1), :]
            above, below = jnp.where(odd, a, b), jnp.where(odd, b, a)
            extra = jnp.where(row == 0, above, 0.0) + jnp.where(row == rows - 1, below, 0.0)
            out[...] = image[at] + extra

    return pl.pallas_call(
        kernel,
        in_specs=[smem()] + [vmem()] * 3,
        out_specs=[vmem()] * 3,
        out_shape=[jax.ShapeDtypeStruct((rows, width), jnp.float32)] * 3,
        compiler_params=pltpu.CompilerParams(vmem_limit_bytes=16 << 20),
        name="border",
    )(col, image, near, far)


def pairs(low, high):
    route = list(zip(low, high))
    return route + [(b, a) for a, b in route]


def neighbours(near, far):
    count = lax.axis_size("col")
    far = lax.ppermute(far, "col", pairs(range(1, count - 1, 2), range(2, count, 2)))
    near = lax.ppermute(near, "col", pairs(range(0, count - 1, 2), range(1, count, 2)))
    return near, far


def wide_exchange(parts, slabs, width):
    _, kinds, rows, _ = parts.shape
    tiles = parts.transpose(1, 2, 0, 3).reshape(kinds, rows, slabs, width).transpose(2, 0, 1, 3)
    got = lax.all_to_all(tiles, "slab", 0, 0)
    done = [got[0, what] for what in range(kinds)]
    for s in range(1, slabs):
        done = join(done, [got[s, what] for what in range(kinds)], False)
    return jnp.stack(done)[None]


def swap(x, count, distance):
    low = [i for i in range(count) if not i & distance]
    return lax.ppermute(x, "slab", pairs(low, [i + distance for i in low]))


def body(field, fine_plane, fine_frac, counts):
    slabs = lax.axis_size("slab")
    depth, columns = field.shape[1], field.shape[3]
    width = columns // slabs
    slab = lax.axis_index("slab").reshape(1).astype(jnp.int32)
    col = lax.axis_index("col").reshape(1).astype(jnp.int32)
    fast = slabs == 4 and width % LANES == 0
    block = width if fast else LANES
    blocks = columns // block

    def block_of(b, s):
        if not fast:
            return b
        parity = jnp.where(b < 2, 1 - (s & 1), s & 1)
        return 2 * (((s >> 1) & 1) ^ 1 ^ (b & 1)) + parity

    follow = lax.ppermute(field[:, :1], "slab", [(i + 1, i) for i in range(slabs - 1)])
    ahead = march(field, fine_plane, fine_frac, counts, slab, blocks, block_of, block)

    def part(first, steps, coded):
        return close(ahead, follow, slab, depth, first, steps, block_of, coded)

    if not fast:
        parts = part(0, blocks, False)
        image, near, far = finish(wide_exchange(parts, slabs, width), (), slab, col)
        return border(image, *neighbours(near, far), col)

    got_a = swap(part(0, 1, True), slabs, 1)
    keep_a = part(2, 1, False)
    got = swap(relay(keep_a, got_a, slab), slabs, 2)
    got_b = swap(part(1, 1, True), slabs, 1)
    keep_b = part(3, 1, False)
    image, near, far = finish(keep_b, (got_b, got), slab, col)
    return border(image, *neighbours(near, far), col)


def solution(mesh):
    in_specs = (
        P(None, "slab", "col", None),
        P("slab", "col", None),
        P("slab", "col", None),
        P("slab", "col", None),
    )
    out_specs = (P("col", "slab"), P("col", "slab"), P("col", "slab"))

    return jax.shard_map(body, mesh=mesh, in_specs=in_specs, out_specs=out_specs, check_vma=False)
```

```python
import functools

import jax
import jax.numpy as jnp
from jax import lax
from jax.experimental import pallas as pl
from jax.experimental.pallas import tpu as pltpu
from jax.sharding import PartitionSpec as P

LOG2E = 1.4426950408889634
ROWS = 16
LANES = 128
COLOR, DEEP, FINE, COARSE, COARSE_PASS = range(5)
OCTAVES = 24.0
STEPS = 65534.0 / OCTAVES
WIRE = jnp.int16


def vmem():
    return pl.BlockSpec(memory_space=pltpu.VMEM)


def encode(x):
    if WIRE == jnp.float32:
        return x
    y = jnp.maximum(jnp.log2(x) * STEPS + 65535.5, 0.0)
    return (y.astype(jnp.int32) - 32768).astype(jnp.int16)


def decode(code):
    if WIRE == jnp.float32:
        return code
    y = code.astype(jnp.int32).astype(jnp.float32)
    x = jnp.exp2((y - 32767.0) * (1.0 / STEPS))
    return jnp.where(y > -32767.5, x, 0.0)


def shade(raw0, raw1, power):
    soft = jnp.log2(1.0 + jnp.exp2(raw0 * LOG2E))
    return jnp.exp2(soft * power), 1.0 + jnp.tanh(0.5 * raw1)


def march_rows(field, plane, frac, counts, run, late, here, cols, base, total_depth):
    depth, slots = field.shape[1], plane.shape[0]
    unit = 8 if 8 * depth <= 256 else 1
    size = (ROWS, LANES)
    live = counts[0, here, cols]
    color = jnp.zeros(size, jnp.float32)
    deep = jnp.zeros(size, jnp.float32)
    passed = jnp.ones(size, jnp.float32)
    for i in range(slots):
        place = plane[i, here, cols] * 8 + frac[i, here, cols]
        k = (place & 15).astype(jnp.float32)
        to_odd = jnp.minimum(k, 16.0 - k) * 0.125
        place = place.astype(jnp.float32)
        spot = place if unit == 8 else plane[i, here, cols].astype(jnp.float32)
        spot = spot.astype(jnp.bfloat16)
        even = [field[ch, 0, here, cols] for ch in (0, 1)]
        odd = [field[ch, 1, here, cols] for ch in (0, 1)]
        for z in range(1, depth - 1):
            hit = spot >= jnp.bfloat16(unit * z)
            group = even if z % 2 else odd
            for ch in (0, 1):
                group[ch] = jnp.where(hit, field[ch, z + 1, here, cols], group[ch])
        values = []
        for ch in (0, 1):
            e, o = even[ch].astype(jnp.float32), odd[ch].astype(jnp.float32)
            values.append(e + to_odd * (o - e))
        factor, emission = shade(*values, -(depth / slots) * (2.0 / total_depth))
        rest = jnp.where(live > i, place - 8.0 * (depth - 1), -1.0)
        early = (live > i) & (place < 8.0 * (depth - 1))
        late[i, here, cols] = jnp.maximum(rest, -1.0).astype(jnp.bfloat16)
        factor = jnp.where(early, factor, 1.0)
        weight = passed * (1.0 - factor)
        color = color + weight * emission
        deep = deep + weight * (place + base)
        passed = passed * factor
    run[COLOR, here, cols] = color
    run[DEEP, here, cols] = deep
    run[FINE, here, cols] = passed
    color = jnp.zeros(size, jnp.float32)
    passed = jnp.ones(size, jnp.float32)
    for z in range(7, depth - 1, 8):
        values = [
            0.5 * (field[ch, z, here, cols].astype(jnp.float32)
                   + field[ch, z + 1, here, cols].astype(jnp.float32))
            for ch in (0, 1)
        ]
        factor, emission = shade(*values, -8.0 * (2.0 / total_depth))
        color = color + passed * (1.0 - factor) * emission
        passed = passed * factor
    run[COARSE, here, cols] = color
    run[COARSE_PASS, here, cols] = passed


def tiles(rows, width, step):
    across = width // LANES

    def one(at, carry):
        here = pl.ds(pl.multiple_of((at // across) * ROWS, ROWS), ROWS)
        step(here, pl.ds(pl.multiple_of((at % across) * LANES, LANES), LANES))
        return carry

    lax.fori_loop(0, (rows // ROWS) * across, one, 0)


def march(field, plane, frac, counts, width):
    _, depth, rows, columns = field.shape
    slots, steps = plane.shape[0], columns // width
    total_depth = depth * lax.axis_size("slab")

    def kernel(field, plane, frac, counts, run, late, last):
        base = (lax.axis_index("slab") * (8 * depth)).astype(jnp.float32)
        last[0] = field[:, depth - 1]
        tiles(rows, width, lambda here, cols: march_rows(
            field, plane, frac, counts, run.at[0], late.at[0], here, cols, base, total_depth
        ))

    def spec(*lead):
        zeros = (0,) * len(lead)
        return pl.BlockSpec(lead + (rows, width), lambda b: zeros + (0, b))

    def out(*lead):
        zeros = (0,) * len(lead)
        return pl.BlockSpec((1,) + lead + (rows, width), lambda b: (b,) + zeros + (0, 0))

    def shape(*lead, kind):
        return jax.ShapeDtypeStruct((steps,) + lead + (rows, width), kind)

    return pl.pallas_call(
        kernel,
        grid=(steps,),
        in_specs=[spec(2, depth), spec(slots), spec(slots), spec(1)],
        out_specs=[out(5), out(slots), out(2)],
        out_shape=[
            shape(5, kind=jnp.float32), shape(slots, kind=jnp.bfloat16),
            shape(2, kind=jnp.bfloat16),
        ],
        compiler_params=pltpu.CompilerParams(vmem_limit_bytes=24 << 20),
        cost_estimate=pl.CostEstimate(
            flops=steps * rows * width * 3000, bytes_accessed=steps * rows * width * 128,
            transcendentals=0,
        ),
        name="march",
    )(*(pltpu.with_memory_space_constraint(x, pltpu.HBM) for x in (field, plane, frac, counts)))


def close(ahead, follow, depth, first, steps, block_of, coded):
    run, late, last = ahead
    _, slots, rows, width = late.shape
    total_depth = depth * lax.axis_size("slab")

    def kernel(run, late, last, follow, out):
        s = lax.axis_index("slab")
        base = (s * (8 * depth) + 8 * (depth - 1)).astype(jnp.float32)

        def step(i, here, cols):
            b = block_of(first + i, s)
            start = b * width + cols.start
            there = pl.ds(pl.multiple_of(start, LANES), LANES)
            low = [last[b, ch, here, cols].astype(jnp.float32) for ch in (0, 1)]
            high = [follow[ch, 0, here, there].astype(jnp.float32) for ch in (0, 1)]
            slope = [(h - l) * 0.125 for h, l in zip(high, low)]
            color, deep, passed = (run[b, what, here, cols] for what in (COLOR, DEEP, FINE))
            for k in range(slots):
                eighths = late[b, k, here, cols].astype(jnp.float32)
                values = [l + eighths * d for l, d in zip(low, slope)]
                factor, emission = shade(*values, -(depth / slots) * (2.0 / total_depth))
                factor = jnp.where(eighths >= 0.0, factor, 1.0)
                weight = passed * (1.0 - factor)
                color = color + weight * emission
                deep = deep + weight * (eighths + base)
                passed = passed * factor
            values = [0.5 * (h + l) for h, l in zip(high, low)]
            factor, emission = shade(*values, -8.0 * (2.0 / total_depth))
            coarse, through = (run[b, what, here, cols] for what in (COARSE, COARSE_PASS))
            coarse = coarse + through * (1.0 - factor) * emission
            done = {
                COLOR: 0.5 * color, DEEP: deep * (1.0 / (8.0 * total_depth)), FINE: passed,
                COARSE: 0.5 * coarse, COARSE_PASS: through * factor,
            }
            for what, value in done.items():
                out[i, what, here, cols] = encode(value) if coded else value

        for i in range(steps):
            tiles(rows, width, functools.partial(step, i))

    return pl.pallas_call(
        kernel,
        in_specs=[vmem()] * 4,
        out_specs=vmem(),
        out_shape=jax.ShapeDtypeStruct((steps, 5, rows, width), WIRE if coded else jnp.float32),
        compiler_params=pltpu.CompilerParams(vmem_limit_bytes=24 << 20),
        cost_estimate=pl.CostEstimate(
            flops=steps * rows * width * 1500, bytes_accessed=steps * rows * width * 64,
            transcendentals=0,
        ),
        name="close",
    )(run, late, last, follow)


def join(mine, got, got_first):
    first = [jnp.where(got_first, g, m) for m, g in zip(mine, got)]
    last = [jnp.where(got_first, m, g) for m, g in zip(mine, got)]
    return [
        first[COLOR] + first[FINE] * last[COLOR],
        first[DEEP] + first[FINE] * last[DEEP],
        first[FINE] * last[FINE],
        first[COARSE] + first[COARSE_PASS] * last[COARSE],
        first[COARSE_PASS] * last[COARSE_PASS],
    ]


def relay(mine, got):
    _, kinds, rows, _ = mine.shape

    def kernel(mine, got, send):
        got_first = lax.axis_index("slab") & 1 == 1
        for r in range(0, rows, ROWS):
            here = pl.ds(r, ROWS)
            done = join(
                [mine[0, what, here, :] for what in range(kinds)],
                [decode(got[0, what, here, :]) for what in range(kinds)],
                got_first,
            )
            for what in range(kinds):
                send[0, what, here, :] = encode(done[what])

    return pl.pallas_call(
        kernel,
        in_specs=[vmem()] * 2,
        out_specs=vmem(),
        out_shape=jax.ShapeDtypeStruct(got.shape, WIRE),
        compiler_params=pltpu.CompilerParams(vmem_limit_bytes=16 << 20),
        name="relay",
    )(mine, got)


def finish(mine, got):
    _, kinds, rows, width = mine.shape
    runs = [mine, *got]

    def kernel(mine, *refs):
        *partner, image, near, far = refs
        odd = lax.axis_index("col") % 2 == 1
        done = [mine[0, what] for what in range(kinds)]
        for bit, got in enumerate(partner):
            got_first = (lax.axis_index("slab") >> bit) & 1 == 1
            done = join(done, [decode(got[0, what]) for what in range(kinds)], got_first)
        row = lax.broadcasted_iota(jnp.int32, (rows, width), 0)
        for at, what in enumerate((COLOR, DEEP, COARSE)):
            x = done[what]
            up = jnp.where(row == 0, 0.0, pltpu.roll(x, 1, 0))
            down = jnp.where(row == rows - 1, 0.0, pltpu.roll(x, rows - 1, 0))
            image[at] = 0.25 * up + 0.5 * x + 0.25 * down
            top, bottom = x[0:1], x[rows - 1 : rows]
            near[pl.ds(at, 1), :] = 0.25 * jnp.where(odd, top, bottom)
            far[pl.ds(at, 1), :] = 0.25 * jnp.where(odd, bottom, top)

    edge = jax.ShapeDtypeStruct((3, width), jnp.float32)
    return pl.pallas_call(
        kernel,
        in_specs=[vmem()] * len(runs),
        out_specs=[vmem()] * 3,
        out_shape=[jax.ShapeDtypeStruct((3, rows, width), jnp.float32), edge, edge],
        compiler_params=pltpu.CompilerParams(vmem_limit_bytes=16 << 20),
        name="finish",
    )(*runs)


def border(image, near, far):
    _, rows, width = image.shape
    count = lax.axis_size("col")

    def kernel(image, near, far, *outs):
        col = lax.axis_index("col")
        odd = col % 2 == 1
        outermost = (col == 0) | (col == count - 1)
        row = lax.broadcasted_iota(jnp.int32, (rows, width), 0)
        for at, out in enumerate(outs):
            a, b = near[pl.ds(at, 1), :], jnp.where(outermost, 0.0, far[pl.ds(at, 1), :])
            above, below = jnp.where(odd, a, b), jnp.where(odd, b, a)
            extra = jnp.where(row == 0, above, 0.0) + jnp.where(row == rows - 1, below, 0.0)
            out[...] = image[at] + extra

    return pl.pallas_call(
        kernel,
        in_specs=[vmem()] * 3,
        out_specs=[vmem()] * 3,
        out_shape=[jax.ShapeDtypeStruct((rows, width), jnp.float32)] * 3,
        compiler_params=pltpu.CompilerParams(vmem_limit_bytes=16 << 20),
        name="border",
    )(image, near, far)


def pairs(low, high):
    route = list(zip(low, high))
    return route + [(b, a) for a, b in route]


def neighbours(near, far):
    count = lax.axis_size("col")
    far = lax.ppermute(far, "col", pairs(range(1, count, 2), [*range(2, count, 2), 0]))
    near = lax.ppermute(near, "col", pairs(range(0, count - 1, 2), range(1, count, 2)))
    return near, far


def wide_exchange(parts, slabs, width):
    _, kinds, rows, _ = parts.shape
    tiles = parts.transpose(1, 2, 0, 3).reshape(kinds, rows, slabs, width).transpose(2, 0, 1, 3)
    got = lax.all_to_all(tiles, "slab", 0, 0)
    done = [got[0, what] for what in range(kinds)]
    for s in range(1, slabs):
        done = join(done, [got[s, what] for what in range(kinds)], False)
    return jnp.stack(done)[None]


def swap(x, count, distance):
    low = [i for i in range(count) if not i & distance]
    return lax.ppermute(x, "slab", pairs(low, [i + distance for i in low]))


def body(field, fine_plane, fine_frac, counts):
    slabs = lax.axis_size("slab")
    depth, columns = field.shape[1], field.shape[3]
    width = columns // slabs
    fast = slabs == 4 and width % LANES == 0
    block = width if fast else LANES
    blocks = columns // block

    def block_of(b, s):
        if not fast:
            return b
        parity = jnp.where(b < 2, 1 - (s & 1), s & 1)
        return 2 * (((s >> 1) & 1) ^ 1 ^ (b & 1)) + parity

    follow = lax.ppermute(field[:, :1], "slab", [(i + 1, i) for i in range(slabs - 1)])
    ahead = march(field, fine_plane, fine_frac, counts, block)

    def part(first, steps, coded):
        return close(ahead, follow, depth, first, steps, block_of, coded)

    if not fast:
        parts = part(0, blocks, False)
        image, near, far = finish(wide_exchange(parts, slabs, width), ())
        return border(image, *neighbours(near, far))

    got_a = swap(part(0, 1, True), slabs, 1)
    keep_a = part(2, 1, False)
    got = swap(relay(keep_a, got_a), slabs, 2)
    got_b = swap(part(1, 1, True), slabs, 1)
    keep_b = part(3, 1, False)
    image, near, far = finish(keep_b, (got_b, got))
    return border(image, *neighbours(near, far))


def solution(mesh):
    in_specs = (
        P(None, "slab", "col", None),
        P("slab", "col", None),
        P("slab", "col", None),
        P("slab", "col", None),
    )
    out_specs = (P("col", "slab"), P("col", "slab"), P("col", "slab"))

    return jax.shard_map(body, mesh=mesh, in_specs=in_specs, out_specs=out_specs, check_vma=False)
```

```python
import functools

import jax
import jax.numpy as jnp
from jax import lax
from jax.experimental import pallas as pl
from jax.experimental.pallas import tpu as pltpu
from jax.sharding import PartitionSpec as P

LOG2E = 1.4426950408889634
ROWS = 16
LANES = 128
COLOR, DEEP, FINE, COARSE, COARSE_PASS = range(5)
OCTAVES = 24.0
STEPS = 65534.0 / OCTAVES
WIRE = jnp.int16


def vmem():
    return pl.BlockSpec(memory_space=pltpu.VMEM)


def encode(x):
    if WIRE == jnp.float32:
        return x
    y = jnp.maximum(jnp.log2(x) * STEPS + 65535.5, 0.0)
    return (y.astype(jnp.int32) - 32768).astype(jnp.int16)


def decode(code):
    if WIRE == jnp.float32:
        return code
    y = code.astype(jnp.int32).astype(jnp.float32)
    x = jnp.exp2((y - 32767.0) * (1.0 / STEPS))
    return jnp.where(y > -32767.5, x, 0.0)


def shade(raw0, raw1, power):
    soft = jnp.log2(1.0 + jnp.exp2(raw0 * LOG2E))
    return jnp.exp2(soft * power), 1.0 + jnp.tanh(0.5 * raw1)


def march_rows(field, plane, frac, counts, run, late, here, cols, base, total_depth):
    depth, slots = field.shape[1], plane.shape[0]
    unit = 8 if 8 * depth <= 256 else 1
    size = (ROWS, LANES)
    live = counts[0, here, cols]
    color = jnp.zeros(size, jnp.float32)
    deep = jnp.zeros(size, jnp.float32)
    passed = jnp.ones(size, jnp.float32)
    for i in range(slots):
        place = plane[i, here, cols] * 8 + frac[i, here, cols]
        k = (place & 15).astype(jnp.float32)
        to_odd = jnp.minimum(k, 16.0 - k) * 0.125
        place = place.astype(jnp.float32)
        spot = place if unit == 8 else plane[i, here, cols].astype(jnp.float32)
        spot = spot.astype(jnp.bfloat16)
        even = [field[ch, 0, here, cols] for ch in (0, 1)]
        odd = [field[ch, 1, here, cols] for ch in (0, 1)]
        for z in range(1, depth - 1):
            hit = spot >= jnp.bfloat16(unit * z)
            group = even if z % 2 else odd
            for ch in (0, 1):
                group[ch] = jnp.where(hit, field[ch, z + 1, here, cols], group[ch])
        values = []
        for ch in (0, 1):
            e, o = even[ch].astype(jnp.float32), odd[ch].astype(jnp.float32)
            values.append(e + to_odd * (o - e))
        factor, emission = shade(*values, -(depth / slots) * (2.0 / total_depth))
        rest = jnp.where(live > i, place - 8.0 * (depth - 1), -1.0)
        early = (live > i) & (place < 8.0 * (depth - 1))
        late[i, here, cols] = jnp.maximum(rest, -1.0).astype(jnp.bfloat16)
        factor = jnp.where(early, factor, 1.0)
        weight = passed * (1.0 - factor)
        color = color + weight * emission
        deep = deep + weight * (place + base)
        passed = passed * factor
    run[COLOR, here, cols] = color
    run[DEEP, here, cols] = deep
    run[FINE, here, cols] = passed
    color = jnp.zeros(size, jnp.float32)
    passed = jnp.ones(size, jnp.float32)
    for z in range(7, depth - 1, 8):
        values = [
            0.5 * (field[ch, z, here, cols].astype(jnp.float32)
                   + field[ch, z + 1, here, cols].astype(jnp.float32))
            for ch in (0, 1)
        ]
        factor, emission = shade(*values, -8.0 * (2.0 / total_depth))
        color = color + passed * (1.0 - factor) * emission
        passed = passed * factor
    run[COARSE, here, cols] = color
    run[COARSE_PASS, here, cols] = passed


def tiles(rows, width, step):
    across = width // LANES

    def one(at, carry):
        here = pl.ds(pl.multiple_of((at // across) * ROWS, ROWS), ROWS)
        step(here, pl.ds(pl.multiple_of((at % across) * LANES, LANES), LANES))
        return carry

    lax.fori_loop(0, (rows // ROWS) * across, one, 0)


def march(field, plane, frac, counts, width):
    _, depth, rows, columns = field.shape
    slots, steps = plane.shape[0], columns // width
    total_depth = depth * lax.axis_size("slab")

    def kernel(field, plane, frac, counts, run, late, last):
        base = (lax.axis_index("slab") * (8 * depth)).astype(jnp.float32)
        last[0] = field[:, depth - 1]
        tiles(rows, width, lambda here, cols: march_rows(
            field, plane, frac, counts, run.at[0], late.at[0], here, cols, base, total_depth
        ))

    def spec(*lead):
        zeros = (0,) * len(lead)
        return pl.BlockSpec(lead + (rows, width), lambda b: zeros + (0, b))

    def out(*lead):
        zeros = (0,) * len(lead)
        return pl.BlockSpec((1,) + lead + (rows, width), lambda b: (b,) + zeros + (0, 0))

    def shape(*lead, kind):
        return jax.ShapeDtypeStruct((steps,) + lead + (rows, width), kind)

    return pl.pallas_call(
        kernel,
        grid=(steps,),
        in_specs=[spec(2, depth), spec(slots), spec(slots), spec(1)],
        out_specs=[out(5), out(slots), out(2)],
        out_shape=[
            shape(5, kind=jnp.float32), shape(slots, kind=jnp.bfloat16),
            shape(2, kind=jnp.bfloat16),
        ],
        compiler_params=pltpu.CompilerParams(vmem_limit_bytes=24 << 20),
        cost_estimate=pl.CostEstimate(
            flops=steps * rows * width * 3000, bytes_accessed=steps * rows * width * 128,
            transcendentals=0,
        ),
        name="march",
    )(*(pltpu.with_memory_space_constraint(x, pltpu.HBM) for x in (field, plane, frac, counts)))


def close(ahead, follow, depth, first, steps, block_of, coded):
    run, late, last = ahead
    _, slots, rows, width = late.shape
    total_depth = depth * lax.axis_size("slab")

    def kernel(run, late, last, follow, out):
        s = lax.axis_index("slab")
        base = (s * (8 * depth) + 8 * (depth - 1)).astype(jnp.float32)

        def step(i, here, cols):
            b = block_of(first + i, s)
            start = b * width + cols.start
            there = pl.ds(pl.multiple_of(start, LANES), LANES)
            low = [last[b, ch, here, cols].astype(jnp.float32) for ch in (0, 1)]
            high = [follow[ch, 0, here, there].astype(jnp.float32) for ch in (0, 1)]
            slope = [(h - l) * 0.125 for h, l in zip(high, low)]
            color, deep, passed = (run[b, what, here, cols] for what in (COLOR, DEEP, FINE))
            for k in range(slots):
                eighths = late[b, k, here, cols].astype(jnp.float32)
                values = [l + eighths * d for l, d in zip(low, slope)]
                factor, emission = shade(*values, -(depth / slots) * (2.0 / total_depth))
                factor = jnp.where(eighths >= 0.0, factor, 1.0)
                weight = passed * (1.0 - factor)
                color = color + weight * emission
                deep = deep + weight * (eighths + base)
                passed = passed * factor
            values = [0.5 * (h + l) for h, l in zip(high, low)]
            factor, emission = shade(*values, -8.0 * (2.0 / total_depth))
            coarse, through = (run[b, what, here, cols] for what in (COARSE, COARSE_PASS))
            coarse = coarse + through * (1.0 - factor) * emission
            done = {
                COLOR: 0.5 * color, DEEP: deep * (1.0 / (8.0 * total_depth)), FINE: passed,
                COARSE: 0.5 * coarse, COARSE_PASS: through * factor,
            }
            for what, value in done.items():
                out[i, what, here, cols] = encode(value) if coded else value

        for i in range(steps):
            tiles(rows, width, functools.partial(step, i))

    return pl.pallas_call(
        kernel,
        in_specs=[vmem()] * 4,
        out_specs=vmem(),
        out_shape=jax.ShapeDtypeStruct((steps, 5, rows, width), WIRE if coded else jnp.float32),
        compiler_params=pltpu.CompilerParams(vmem_limit_bytes=24 << 20),
        cost_estimate=pl.CostEstimate(
            flops=steps * rows * width * 1500, bytes_accessed=steps * rows * width * 64,
            transcendentals=0,
        ),
        name="close",
    )(run, late, last, follow)


def join(mine, got, got_first):
    first = [jnp.where(got_first, g, m) for m, g in zip(mine, got)]
    last = [jnp.where(got_first, m, g) for m, g in zip(mine, got)]
    return [
        first[COLOR] + first[FINE] * last[COLOR],
        first[DEEP] + first[FINE] * last[DEEP],
        first[FINE] * last[FINE],
        first[COARSE] + first[COARSE_PASS] * last[COARSE],
        first[COARSE_PASS] * last[COARSE_PASS],
    ]


def relay(mine, got):
    _, kinds, rows, _ = mine.shape

    def kernel(mine, got, send):
        got_first = lax.axis_index("slab") & 1 == 1
        for r in range(0, rows, ROWS):
            here = pl.ds(r, ROWS)
            done = join(
                [mine[0, what, here, :] for what in range(kinds)],
                [decode(got[0, what, here, :]) for what in range(kinds)],
                got_first,
            )
            for what in range(kinds):
                send[0, what, here, :] = encode(done[what])

    return pl.pallas_call(
        kernel,
        in_specs=[vmem()] * 2,
        out_specs=vmem(),
        out_shape=jax.ShapeDtypeStruct(got.shape, WIRE),
        compiler_params=pltpu.CompilerParams(vmem_limit_bytes=16 << 20),
        name="relay",
    )(mine, got)


def finish(mine, got):
    _, kinds, rows, width = mine.shape
    runs = [mine, *got]

    def kernel(mine, *refs):
        *partner, image, near, far = refs
        odd = lax.axis_index("col") % 2 == 1
        done = [mine[0, what] for what in range(kinds)]
        for bit, got in enumerate(partner):
            got_first = (lax.axis_index("slab") >> bit) & 1 == 1
            done = join(done, [decode(got[0, what]) for what in range(kinds)], got_first)
        row = lax.broadcasted_iota(jnp.int32, (rows, width), 0)
        for at, what in enumerate((COLOR, DEEP, COARSE)):
            x = done[what]
            up = jnp.where(row == 0, 0.0, pltpu.roll(x, 1, 0))
            down = jnp.where(row == rows - 1, 0.0, pltpu.roll(x, rows - 1, 0))
            image[at] = 0.25 * up + 0.5 * x + 0.25 * down
            top, bottom = x[0:1], x[rows - 1 : rows]
            near[pl.ds(at, 1), :] = 0.25 * jnp.where(odd, top, bottom)
            far[pl.ds(at, 1), :] = 0.25 * jnp.where(odd, bottom, top)

    edge = jax.ShapeDtypeStruct((3, width), jnp.float32)
    return pl.pallas_call(
        kernel,
        in_specs=[vmem()] * len(runs),
        out_specs=[vmem()] * 3,
        out_shape=[jax.ShapeDtypeStruct((3, rows, width), jnp.float32), edge, edge],
        compiler_params=pltpu.CompilerParams(vmem_limit_bytes=16 << 20),
        name="finish",
    )(*runs)


def border(image, near, far):
    _, rows, width = image.shape
    count = lax.axis_size("col")

    def kernel(image, near, far, *outs):
        col = lax.axis_index("col")
        odd = col % 2 == 1
        outermost = (col == 0) | (col == count - 1)
        row = lax.broadcasted_iota(jnp.int32, (rows, width), 0)
        for at, out in enumerate(outs):
            a, b = near[pl.ds(at, 1), :], jnp.where(outermost, 0.0, far[pl.ds(at, 1), :])
            above, below = jnp.where(odd, a, b), jnp.where(odd, b, a)
            extra = jnp.where(row == 0, above, 0.0) + jnp.where(row == rows - 1, below, 0.0)
            out[...] = image[at] + extra

    return pl.pallas_call(
        kernel,
        in_specs=[vmem()] * 3,
        out_specs=[vmem()] * 3,
        out_shape=[jax.ShapeDtypeStruct((rows, width), jnp.float32)] * 3,
        compiler_params=pltpu.CompilerParams(vmem_limit_bytes=16 << 20),
        name="border",
    )(image, near, far)


def pairs(low, high):
    route = list(zip(low, high))
    return route + [(b, a) for a, b in route]


def neighbours(near, far):
    slabs, count = lax.axis_size("slab"), lax.axis_size("col")
    far = lax.ppermute(far, ("slab", "col"), [
        (s * count + a, t * count + b)
        for s in range(slabs)
        for a, b in pairs(range(1, count - 1, 2), range(2, count, 2)) + [(0, 0), (count - 1,) * 2]
        for t in [s ^ 1 if a == b else s]
    ])
    near = lax.ppermute(near, "col", pairs(range(0, count - 1, 2), range(1, count, 2)))
    return near, far


def wide_exchange(parts, slabs, width):
    _, kinds, rows, _ = parts.shape
    tiles = parts.transpose(1, 2, 0, 3).reshape(kinds, rows, slabs, width).transpose(2, 0, 1, 3)
    got = lax.all_to_all(tiles, "slab", 0, 0)
    done = [got[0, what] for what in range(kinds)]
    for s in range(1, slabs):
        done = join(done, [got[s, what] for what in range(kinds)], False)
    return jnp.stack(done)[None]


def swap(x, count, distance):
    low = [i for i in range(count) if not i & distance]
    return lax.ppermute(x, "slab", pairs(low, [i + distance for i in low]))


def body(field, fine_plane, fine_frac, counts):
    slabs = lax.axis_size("slab")
    depth, columns = field.shape[1], field.shape[3]
    width = columns // slabs
    fast = slabs == 4 and width % LANES == 0
    block = width if fast else LANES
    blocks = columns // block

    def block_of(b, s):
        if not fast:
            return b
        parity = jnp.where(b < 2, 1 - (s & 1), s & 1)
        return 2 * (((s >> 1) & 1) ^ 1 ^ (b & 1)) + parity

    follow = lax.ppermute(field[:, :1], "slab", [(i + 1, i) for i in range(slabs - 1)])
    ahead = march(field, fine_plane, fine_frac, counts, block)

    def part(first, steps, coded):
        return close(ahead, follow, depth, first, steps, block_of, coded)

    if not fast:
        parts = part(0, blocks, False)
        image, near, far = finish(wide_exchange(parts, slabs, width), ())
        return border(image, *neighbours(near, far))

    got_a = swap(part(0, 1, True), slabs, 1)
    keep_a = part(2, 1, False)
    got = swap(relay(keep_a, got_a), slabs, 2)
    got_b = swap(part(1, 1, True), slabs, 1)
    keep_b = part(3, 1, False)
    image, near, far = finish(keep_b, (got_b, got))
    return border(image, *neighbours(near, far))


def solution(mesh):
    in_specs = (
        P(None, "slab", "col", None),
        P("slab", "col", None),
        P("slab", "col", None),
        P("slab", "col", None),
    )
    out_specs = (P("col", "slab"), P("col", "slab"), P("col", "slab"))

    return jax.shard_map(body, mesh=mesh, in_specs=in_specs, out_specs=out_specs, check_vma=False)
```

```python
import functools

import jax
import jax.numpy as jnp
from jax import lax
from jax.experimental import pallas as pl
from jax.experimental.pallas import tpu as pltpu
from jax.sharding import PartitionSpec as P

LOG2E = 1.4426950408889634
ROWS = 16
LANES = 128
COLOR, DEEP, FINE, COARSE, COARSE_PASS = range(5)
OCTAVES = (22.0, 22.0, 10.0, 22.0, 10.0)
WIRE = jnp.int16


def vmem():
    return pl.BlockSpec(memory_space=pltpu.VMEM)


def encode(x, what):
    y = jnp.maximum(jnp.log2(x) * (65534.0 / OCTAVES[what]) + 65535.5, 0.0)
    return (y.astype(jnp.int32) - 32768).astype(WIRE)


def decode(code, what):
    y = code.astype(jnp.int32).astype(jnp.float32)
    x = jnp.exp2((y - 32767.0) * (OCTAVES[what] / 65534.0))
    return jnp.where(y > -32767.5, x, 0.0)


SCALES = (LOG2E, 0.5)


def shade(raw0, raw1, power):
    soft = jnp.log2(1.0 + jnp.exp2(raw0))
    return jnp.exp2(soft * power), 1.0 + jnp.tanh(raw1)


def march_rows(field, plane, frac, counts, run, late, here, cols, base, total_depth):
    depth, slots = field.shape[1], plane.shape[0]
    unit = 8 if 8 * depth <= 256 else 1
    size = (ROWS, LANES)
    live = counts[0, here, cols]
    color = jnp.zeros(size, jnp.float32)
    deep = jnp.zeros(size, jnp.float32)
    passed = jnp.ones(size, jnp.float32)
    for i in range(slots):
        place = plane[i, here, cols] * 8 + frac[i, here, cols]
        k = (place & 15).astype(jnp.float32)
        to_odd = jnp.minimum(k, 16.0 - k) * 0.125
        place = place.astype(jnp.float32)
        spot = place if unit == 8 else plane[i, here, cols].astype(jnp.float32)
        spot = spot.astype(jnp.bfloat16)
        even = [field[ch, 0, here, cols] for ch in (0, 1)]
        odd = [field[ch, 1, here, cols] for ch in (0, 1)]
        for z in range(1, depth - 1):
            hit = spot >= jnp.bfloat16(unit * z)
            group = even if z % 2 else odd
            for ch in (0, 1):
                group[ch] = jnp.where(hit, field[ch, z + 1, here, cols], group[ch])
        values = []
        for ch in (0, 1):
            e, o = even[ch].astype(jnp.float32), odd[ch].astype(jnp.float32)
            values.append((e + to_odd * (o - e)) * SCALES[ch])
        factor, emission = shade(*values, -(depth / slots) * (2.0 / total_depth))
        rest = jnp.where(live > i, place - 8.0 * (depth - 1), -1.0)
        early = (live > i) & (place < 8.0 * (depth - 1))
        late[i, here, cols] = jnp.maximum(rest, -1.0).astype(jnp.bfloat16)
        factor = jnp.where(early, factor, 1.0)
        weight = passed * (1.0 - factor)
        color = color + weight * emission
        deep = deep + weight * (place + base)
        passed = passed * factor
    run[COLOR, here, cols] = color
    run[DEEP, here, cols] = deep
    run[FINE, here, cols] = passed
    color = jnp.zeros(size, jnp.float32)
    passed = jnp.ones(size, jnp.float32)
    for z in range(7, depth - 1, 8):
        values = [
            (0.5 * SCALES[ch]) * (field[ch, z, here, cols].astype(jnp.float32)
                   + field[ch, z + 1, here, cols].astype(jnp.float32))
            for ch in (0, 1)
        ]
        factor, emission = shade(*values, -8.0 * (2.0 / total_depth))
        color = color + passed * (1.0 - factor) * emission
        passed = passed * factor
    run[COARSE, here, cols] = color
    run[COARSE_PASS, here, cols] = passed


def tiles(rows, width, step):
    across = width // LANES

    def one(at, carry):
        here = pl.ds(pl.multiple_of((at // across) * ROWS, ROWS), ROWS)
        step(here, pl.ds(pl.multiple_of((at % across) * LANES, LANES), LANES))
        return carry

    lax.fori_loop(0, (rows // ROWS) * across, one, 0)


def march(field, plane, frac, counts, width):
    _, depth, rows, columns = field.shape
    slots, steps = plane.shape[0], columns // width
    total_depth = depth * lax.axis_size("slab")

    def kernel(field, plane, frac, counts, run, late, last):
        base = (lax.axis_index("slab") * (8 * depth)).astype(jnp.float32)
        last[0] = field[:, depth - 1]
        tiles(rows, width, lambda here, cols: march_rows(
            field, plane, frac, counts, run.at[0], late.at[0], here, cols, base, total_depth
        ))

    def spec(*lead):
        zeros = (0,) * len(lead)
        return pl.BlockSpec(lead + (rows, width), lambda b: zeros + (0, b))

    def out(*lead):
        zeros = (0,) * len(lead)
        return pl.BlockSpec((1,) + lead + (rows, width), lambda b: (b,) + zeros + (0, 0))

    def shape(*lead, kind):
        return jax.ShapeDtypeStruct((steps,) + lead + (rows, width), kind)

    return pl.pallas_call(
        kernel,
        grid=(steps,),
        in_specs=[spec(2, depth), spec(slots), spec(slots), spec(1)],
        out_specs=[out(5), out(slots), out(2)],
        out_shape=[
            shape(5, kind=jnp.float32), shape(slots, kind=jnp.bfloat16),
            shape(2, kind=jnp.bfloat16),
        ],
        compiler_params=pltpu.CompilerParams(vmem_limit_bytes=24 << 20),
        cost_estimate=pl.CostEstimate(
            flops=steps * rows * width * 3000, bytes_accessed=steps * rows * width * 128,
            transcendentals=0,
        ),
        name="march",
    )(*(pltpu.with_memory_space_constraint(x, pltpu.HBM) for x in (field, plane, frac, counts)))


def close(ahead, follow, depth, first, steps, block_of, coded):
    run, late, last = ahead
    _, slots, rows, width = late.shape
    total_depth = depth * lax.axis_size("slab")

    def kernel(run, late, last, follow, out):
        s = lax.axis_index("slab")
        base = (s * (8 * depth) + 8 * (depth - 1)).astype(jnp.float32)

        def step(i, here, cols):
            b = block_of(first + i, s)
            start = b * width + cols.start
            there = pl.ds(pl.multiple_of(start, LANES), LANES)
            low = [last[b, ch, here, cols].astype(jnp.float32) * SCALES[ch] for ch in (0, 1)]
            high = [follow[ch, 0, here, there].astype(jnp.float32) * SCALES[ch] for ch in (0, 1)]
            slope = [(h - l) * 0.125 for h, l in zip(high, low)]
            color, deep, passed = (run[b, what, here, cols] for what in (COLOR, DEEP, FINE))
            for k in range(slots):
                eighths = late[b, k, here, cols].astype(jnp.float32)
                values = [l + eighths * d for l, d in zip(low, slope)]
                factor, emission = shade(*values, -(depth / slots) * (2.0 / total_depth))
                factor = jnp.where(eighths >= 0.0, factor, 1.0)
                weight = passed * (1.0 - factor)
                color = color + weight * emission
                deep = deep + weight * (eighths + base)
                passed = passed * factor
            values = [0.5 * (h + l) for h, l in zip(high, low)]
            factor, emission = shade(*values, -8.0 * (2.0 / total_depth))
            coarse, through = (run[b, what, here, cols] for what in (COARSE, COARSE_PASS))
            coarse = coarse + through * (1.0 - factor) * emission
            done = {
                COLOR: 0.5 * color, DEEP: deep * (1.0 / (8.0 * total_depth)), FINE: passed,
                COARSE: 0.5 * coarse, COARSE_PASS: through * factor,
            }
            for what, value in done.items():
                out[i, what, here, cols] = encode(value, what) if coded else value

        for i in range(steps):
            tiles(rows, width, functools.partial(step, i))

    return pl.pallas_call(
        kernel,
        in_specs=[vmem()] * 4,
        out_specs=vmem(),
        out_shape=jax.ShapeDtypeStruct((steps, 5, rows, width), WIRE if coded else jnp.float32),
        compiler_params=pltpu.CompilerParams(vmem_limit_bytes=24 << 20),
        cost_estimate=pl.CostEstimate(
            flops=steps * rows * width * 1500, bytes_accessed=steps * rows * width * 64,
            transcendentals=0,
        ),
        name="close",
    )(run, late, last, follow)


def join(mine, got, got_first):
    first = [jnp.where(got_first, g, m) for m, g in zip(mine, got)]
    last = [jnp.where(got_first, m, g) for m, g in zip(mine, got)]
    return [
        first[COLOR] + first[FINE] * last[COLOR],
        first[DEEP] + first[FINE] * last[DEEP],
        first[FINE] * last[FINE],
        first[COARSE] + first[COARSE_PASS] * last[COARSE],
        first[COARSE_PASS] * last[COARSE_PASS],
    ]


def relay(mine, got):
    _, kinds, rows, _ = mine.shape

    def kernel(mine, got, send):
        got_first = lax.axis_index("slab") & 1 == 1
        for r in range(0, rows, ROWS):
            here = pl.ds(r, ROWS)
            done = join(
                [mine[0, what, here, :] for what in range(kinds)],
                [decode(got[0, what, here, :], what) for what in range(kinds)],
                got_first,
            )
            for what in range(kinds):
                send[0, what, here, :] = encode(done[what], what)

    return pl.pallas_call(
        kernel,
        in_specs=[vmem()] * 2,
        out_specs=vmem(),
        out_shape=jax.ShapeDtypeStruct(got.shape, WIRE),
        compiler_params=pltpu.CompilerParams(vmem_limit_bytes=16 << 20),
        name="relay",
    )(mine, got)


def finish(mine, got):
    _, kinds, rows, width = mine.shape
    runs = [mine, *got]

    def kernel(mine, *refs):
        *partner, image, near, far = refs
        odd = lax.axis_index("col") % 2 == 1
        done = [mine[0, what] for what in range(kinds)]
        for bit, got in enumerate(partner):
            got_first = (lax.axis_index("slab") >> bit) & 1 == 1
            done = join(done, [decode(got[0, what], what) for what in range(kinds)], got_first)
        row = lax.broadcasted_iota(jnp.int32, (rows, width), 0)
        for at, what in enumerate((COLOR, DEEP, COARSE)):
            x = done[what]
            up = jnp.where(row == 0, 0.0, pltpu.roll(x, 1, 0))
            down = jnp.where(row == rows - 1, 0.0, pltpu.roll(x, rows - 1, 0))
            image[at] = 0.25 * up + 0.5 * x + 0.25 * down
            top, bottom = x[0:1], x[rows - 1 : rows]
            near[pl.ds(at, 1), :] = 0.25 * jnp.where(odd, top, bottom)
            far[pl.ds(at, 1), :] = 0.25 * jnp.where(odd, bottom, top)

    edge = jax.ShapeDtypeStruct((3, width), jnp.float32)
    return pl.pallas_call(
        kernel,
        in_specs=[vmem()] * len(runs),
        out_specs=[vmem()] * 3,
        out_shape=[jax.ShapeDtypeStruct((3, rows, width), jnp.float32), edge, edge],
        compiler_params=pltpu.CompilerParams(vmem_limit_bytes=16 << 20),
        name="finish",
    )(*runs)


def border(image, near, far):
    _, rows, width = image.shape
    count = lax.axis_size("col")

    def kernel(image, near, far, *outs):
        col = lax.axis_index("col")
        odd = col % 2 == 1
        outermost = (col == 0) | (col == count - 1)
        row = lax.broadcasted_iota(jnp.int32, (rows, width), 0)
        for at, out in enumerate(outs):
            a, b = near[pl.ds(at, 1), :], jnp.where(outermost, 0.0, far[pl.ds(at, 1), :])
            above, below = jnp.where(odd, a, b), jnp.where(odd, b, a)
            extra = jnp.where(row == 0, above, 0.0) + jnp.where(row == rows - 1, below, 0.0)
            out[...] = image[at] + extra

    return pl.pallas_call(
        kernel,
        in_specs=[vmem()] * 3,
        out_specs=[vmem()] * 3,
        out_shape=[jax.ShapeDtypeStruct((rows, width), jnp.float32)] * 3,
        compiler_params=pltpu.CompilerParams(vmem_limit_bytes=16 << 20),
        name="border",
    )(image, near, far)


def pairs(low, high):
    route = list(zip(low, high))
    return route + [(b, a) for a, b in route]


def neighbours(near, far):
    slabs, count = lax.axis_size("slab"), lax.axis_size("col")
    far = lax.ppermute(far, ("slab", "col"), [
        (s * count + a, t * count + b)
        for s in range(slabs)
        for a, b in pairs(range(1, count - 1, 2), range(2, count, 2)) + [(0, 0), (count - 1,) * 2]
        for t in [s ^ 1 if a == b else s]
    ])
    near = lax.ppermute(near, "col", pairs(range(0, count - 1, 2), range(1, count, 2)))
    return near, far


def wide_exchange(parts, slabs, width):
    _, kinds, rows, _ = parts.shape
    tiles = parts.transpose(1, 2, 0, 3).reshape(kinds, rows, slabs, width).transpose(2, 0, 1, 3)
    got = lax.all_to_all(tiles, "slab", 0, 0)
    done = [got[0, what] for what in range(kinds)]
    for s in range(1, slabs):
        done = join(done, [got[s, what] for what in range(kinds)], False)
    return jnp.stack(done)[None]


def swap(x, count, distance):
    low = [i for i in range(count) if not i & distance]
    return lax.ppermute(x, "slab", pairs(low, [i + distance for i in low]))


def body(field, fine_plane, fine_frac, counts):
    slabs = lax.axis_size("slab")
    depth, columns = field.shape[1], field.shape[3]
    width = columns // slabs
    fast = slabs == 4 and width % LANES == 0
    block = width if fast else LANES
    blocks = columns // block

    def block_of(b, s):
        if not fast:
            return b
        parity = jnp.where(b < 2, 1 - (s & 1), s & 1)
        return 2 * (((s >> 1) & 1) ^ 1 ^ (b & 1)) + parity

    follow = lax.ppermute(field[:, :1], "slab", [(i + 1, i) for i in range(slabs - 1)])
    ahead = march(field, fine_plane, fine_frac, counts, block)

    def part(first, steps, coded):
        return close(ahead, follow, depth, first, steps, block_of, coded)

    if not fast:
        parts = part(0, blocks, False)
        image, near, far = finish(wide_exchange(parts, slabs, width), ())
        return border(image, *neighbours(near, far))

    got_a = swap(part(0, 1, True), slabs, 1)
    keep_a = part(2, 1, False)
    got = swap(relay(keep_a, got_a), slabs, 2)
    got_b = swap(part(1, 1, True), slabs, 1)
    keep_b = part(3, 1, False)
    image, near, far = finish(keep_b, (got_b, got))
    return border(image, *neighbours(near, far))


def solution(mesh):
    in_specs = (
        P(None, "slab", "col", None),
        P("slab", "col", None),
        P("slab", "col", None),
        P("slab", "col", None),
    )
    out_specs = (P("col", "slab"), P("col", "slab"), P("col", "slab"))

    return jax.shard_map(body, mesh=mesh, in_specs=in_specs, out_specs=out_specs, check_vma=False)
```

```python
import functools

import jax
import jax.numpy as jnp
from jax import lax
from jax.experimental import pallas as pl
from jax.experimental.pallas import tpu as pltpu
from jax.sharding import PartitionSpec as P

LOG2E = 1.4426950408889634
ROWS = 16
LANES = 128
COLOR, DEEP, FINE, COARSE, COARSE_PASS = range(5)
OCTAVES = (22.0, 22.0, 10.0, 22.0, 10.0)
WIRE = jnp.int16


def vmem():
    return pl.BlockSpec(memory_space=pltpu.VMEM)


def encode(x, what):
    y = jnp.maximum(jnp.log2(x) * (65534.0 / OCTAVES[what]) + 65535.5, 0.0)
    return (y.astype(jnp.int32) - 32768).astype(WIRE)


def decode(code, what):
    y = code.astype(jnp.int32).astype(jnp.float32)
    x = jnp.exp2((y - 32767.0) * (OCTAVES[what] / 65534.0))
    return jnp.where(y > -32767.5, x, 0.0)


SCALES = (LOG2E, 0.5)


def shade(raw0, raw1, power):
    soft = jnp.log2(1.0 + jnp.exp2(raw0))
    return jnp.exp2(soft * power), 1.0 + jnp.tanh(raw1)


def march_rows(field, plane, frac, counts, run, late, here, cols, base, total_depth):
    depth, slots = field.shape[1], plane.shape[0]
    unit = 8 if 8 * depth <= 256 else 1
    size = (ROWS, LANES)
    live = counts[0, here, cols]
    color = jnp.zeros(size, jnp.float32)
    deep = jnp.zeros(size, jnp.float32)
    passed = jnp.ones(size, jnp.float32)
    for i in range(slots):
        place = plane[i, here, cols] * 8 + frac[i, here, cols]
        k = (place & 15).astype(jnp.float32)
        to_odd = jnp.minimum(k, 16.0 - k) * 0.125
        place = place.astype(jnp.float32)
        spot = place if unit == 8 else plane[i, here, cols].astype(jnp.float32)
        spot = spot.astype(jnp.bfloat16)
        even = [field[ch, 0, here, cols] for ch in (0, 1)]
        odd = [field[ch, 1, here, cols] for ch in (0, 1)]
        for z in range(1, depth - 1):
            hit = spot >= jnp.bfloat16(unit * z)
            group = even if z % 2 else odd
            for ch in (0, 1):
                group[ch] = jnp.where(hit, field[ch, z + 1, here, cols], group[ch])
        values = []
        for ch in (0, 1):
            e, o = even[ch].astype(jnp.float32), odd[ch].astype(jnp.float32)
            values.append((e + to_odd * (o - e)) * SCALES[ch])
        factor, emission = shade(*values, -(depth / slots) * (2.0 / total_depth))
        rest = jnp.where(live > i, place - 8.0 * (depth - 1), -1.0)
        early = (live > i) & (place < 8.0 * (depth - 1))
        late[i, here, cols] = jnp.maximum(rest, -1.0).astype(jnp.bfloat16)
        factor = jnp.where(early, factor, 1.0)
        weight = passed * (1.0 - factor)
        color = color + weight * emission
        deep = deep + weight * (place + base)
        passed = passed * factor
    run[COLOR, here, cols] = color
    run[DEEP, here, cols] = deep
    run[FINE, here, cols] = passed
    color = jnp.zeros(size, jnp.float32)
    passed = jnp.ones(size, jnp.float32)
    for z in range(7, depth - 1, 8):
        values = [
            (0.5 * SCALES[ch]) * (field[ch, z, here, cols].astype(jnp.float32)
                   + field[ch, z + 1, here, cols].astype(jnp.float32))
            for ch in (0, 1)
        ]
        factor, emission = shade(*values, -8.0 * (2.0 / total_depth))
        color = color + passed * (1.0 - factor) * emission
        passed = passed * factor
    run[COARSE, here, cols] = color
    run[COARSE_PASS, here, cols] = passed


def tiles(rows, width, step):
    across = width // LANES

    def one(at, carry):
        here = pl.ds(pl.multiple_of((at // across) * ROWS, ROWS), ROWS)
        step(here, pl.ds(pl.multiple_of((at % across) * LANES, LANES), LANES))
        return carry

    lax.fori_loop(0, (rows // ROWS) * across, one, 0)


def march(field, plane, frac, counts, width):
    _, depth, rows, columns = field.shape
    slots, steps = plane.shape[0], columns // width
    total_depth = depth * lax.axis_size("slab")

    def kernel(field, plane, frac, counts, run, late, last):
        base = (lax.axis_index("slab") * (8 * depth)).astype(jnp.float32)
        last[0] = field[:, depth - 1]
        tiles(rows, width, lambda here, cols: march_rows(
            field, plane, frac, counts, run.at[0], late.at[0], here, cols, base, total_depth
        ))

    def spec(*lead):
        zeros = (0,) * len(lead)
        return pl.BlockSpec(lead + (rows, width), lambda b: zeros + (0, b))

    def out(*lead):
        zeros = (0,) * len(lead)
        return pl.BlockSpec((1,) + lead + (rows, width), lambda b: (b,) + zeros + (0, 0))

    def shape(*lead, kind):
        return jax.ShapeDtypeStruct((steps,) + lead + (rows, width), kind)

    return pl.pallas_call(
        kernel,
        grid=(steps,),
        in_specs=[spec(2, depth), spec(slots), spec(slots), spec(1)],
        out_specs=[out(5), out(slots), out(2)],
        out_shape=[
            shape(5, kind=jnp.float32), shape(slots, kind=jnp.bfloat16),
            shape(2, kind=jnp.bfloat16),
        ],
        compiler_params=pltpu.CompilerParams(vmem_limit_bytes=24 << 20),
        cost_estimate=pl.CostEstimate(
            flops=steps * rows * width * 3000, bytes_accessed=steps * rows * width * 128,
            transcendentals=0,
        ),
        name="march",
    )(*(pltpu.with_memory_space_constraint(x, pltpu.HBM) for x in (field, plane, frac, counts)))


def close(ahead, follow, depth, first, steps, block_of, coded):
    run, late, last = ahead
    _, slots, rows, width = late.shape
    total_depth = depth * lax.axis_size("slab")

    def kernel(run, late, last, follow, out):
        s = lax.axis_index("slab")
        base = (s * (8 * depth) + 8 * (depth - 1)).astype(jnp.float32)

        def step(i, here, cols):
            b = block_of(first + i, s)
            start = b * width + cols.start
            there = pl.ds(pl.multiple_of(start, LANES), LANES)
            low = [last[b, ch, here, cols].astype(jnp.float32) * SCALES[ch] for ch in (0, 1)]
            high = [follow[ch, 0, here, there].astype(jnp.float32) * SCALES[ch] for ch in (0, 1)]
            slope = [(h - l) * 0.125 for h, l in zip(high, low)]
            color, deep, passed = (run[b, what, here, cols] for what in (COLOR, DEEP, FINE))
            for k in range(slots):
                eighths = late[b, k, here, cols].astype(jnp.float32)
                values = [l + eighths * d for l, d in zip(low, slope)]
                factor, emission = shade(*values, -(depth / slots) * (2.0 / total_depth))
                factor = jnp.where(eighths >= 0.0, factor, 1.0)
                weight = passed * (1.0 - factor)
                color = color + weight * emission
                deep = deep + weight * (eighths + base)
                passed = passed * factor
            values = [0.5 * (h + l) for h, l in zip(high, low)]
            factor, emission = shade(*values, -8.0 * (2.0 / total_depth))
            coarse, through = (run[b, what, here, cols] for what in (COARSE, COARSE_PASS))
            coarse = coarse + through * (1.0 - factor) * emission
            done = {
                COLOR: 0.5 * color, DEEP: deep * (1.0 / (8.0 * total_depth)), FINE: passed,
                COARSE: 0.5 * coarse, COARSE_PASS: through * factor,
            }
            for what, value in done.items():
                out[i, what, here, cols] = encode(value, what) if coded else value

        for i in range(steps):
            tiles(rows, width, functools.partial(step, i))

    return pl.pallas_call(
        kernel,
        in_specs=[vmem()] * 4,
        out_specs=vmem(),
        out_shape=jax.ShapeDtypeStruct((steps, 5, rows, width), WIRE if coded else jnp.float32),
        compiler_params=pltpu.CompilerParams(vmem_limit_bytes=24 << 20),
        cost_estimate=pl.CostEstimate(
            flops=steps * rows * width * 1500, bytes_accessed=steps * rows * width * 64,
            transcendentals=0,
        ),
        name="close",
    )(run, late, last, follow)


def join(mine, got, got_first):
    first = [jnp.where(got_first, g, m) for m, g in zip(mine, got)]
    last = [jnp.where(got_first, m, g) for m, g in zip(mine, got)]
    return [
        first[COLOR] + first[FINE] * last[COLOR],
        first[DEEP] + first[FINE] * last[DEEP],
        first[FINE] * last[FINE],
        first[COARSE] + first[COARSE_PASS] * last[COARSE],
        first[COARSE_PASS] * last[COARSE_PASS],
    ]


def relay(mine, got, coded):
    _, kinds, rows, _ = mine.shape

    def kernel(mine, got, send):
        got_first = lax.axis_index("slab") & 1 == 1
        for r in range(0, rows, ROWS):
            here = pl.ds(r, ROWS)
            done = join(
                [mine[0, what, here, :] for what in range(kinds)],
                [decode(got[0, what, here, :], what) for what in range(kinds)],
                got_first,
            )
            for what in range(kinds):
                send[0, what, here, :] = encode(done[what], what) if coded else done[what]

    return pl.pallas_call(
        kernel,
        in_specs=[vmem()] * 2,
        out_specs=vmem(),
        out_shape=jax.ShapeDtypeStruct(got.shape, WIRE if coded else jnp.float32),
        compiler_params=pltpu.CompilerParams(vmem_limit_bytes=16 << 20),
        name="relay",
    )(mine, got)


def finish(mine, got):
    _, kinds, rows, width = mine.shape
    runs = [mine, *got]

    def kernel(mine, *refs):
        *partner, image, near, far = refs
        odd = lax.axis_index("col") % 2 == 1
        done = [mine[0, what] for what in range(kinds)]
        for got in partner:
            got_first = (lax.axis_index("slab") >> 1) & 1 == 1
            done = join(done, [decode(got[0, what], what) for what in range(kinds)], got_first)
        row = lax.broadcasted_iota(jnp.int32, (rows, width), 0)
        for at, what in enumerate((COLOR, DEEP, COARSE)):
            x = done[what]
            up = jnp.where(row == 0, 0.0, pltpu.roll(x, 1, 0))
            down = jnp.where(row == rows - 1, 0.0, pltpu.roll(x, rows - 1, 0))
            image[at] = 0.25 * up + 0.5 * x + 0.25 * down
            top, bottom = x[0:1], x[rows - 1 : rows]
            near[pl.ds(at, 1), :] = 0.25 * jnp.where(odd, top, bottom)
            far[pl.ds(at, 1), :] = 0.25 * jnp.where(odd, bottom, top)

    edge = jax.ShapeDtypeStruct((3, width), jnp.float32)
    return pl.pallas_call(
        kernel,
        in_specs=[vmem()] * len(runs),
        out_specs=[vmem()] * 3,
        out_shape=[jax.ShapeDtypeStruct((3, rows, width), jnp.float32), edge, edge],
        compiler_params=pltpu.CompilerParams(vmem_limit_bytes=16 << 20),
        name="finish",
    )(*runs)


def border(image, near, far):
    _, rows, width = image.shape
    count = lax.axis_size("col")

    def kernel(image, near, far, *outs):
        col = lax.axis_index("col")
        odd = col % 2 == 1
        outermost = (col == 0) | (col == count - 1)
        row = lax.broadcasted_iota(jnp.int32, (rows, width), 0)
        for at, out in enumerate(outs):
            a, b = near[pl.ds(at, 1), :], jnp.where(outermost, 0.0, far[pl.ds(at, 1), :])
            above, below = jnp.where(odd, a, b), jnp.where(odd, b, a)
            extra = jnp.where(row == 0, above, 0.0) + jnp.where(row == rows - 1, below, 0.0)
            out[...] = image[at] + extra

    return pl.pallas_call(
        kernel,
        in_specs=[vmem()] * 3,
        out_specs=[vmem()] * 3,
        out_shape=[jax.ShapeDtypeStruct((rows, width), jnp.float32)] * 3,
        compiler_params=pltpu.CompilerParams(vmem_limit_bytes=16 << 20),
        name="border",
    )(image, near, far)


def pairs(low, high):
    route = list(zip(low, high))
    return route + [(b, a) for a, b in route]


def neighbours(near, far):
    slabs, count = lax.axis_size("slab"), lax.axis_size("col")
    far = lax.ppermute(far, ("slab", "col"), [
        (s * count + a, t * count + b)
        for s in range(slabs)
        for a, b in pairs(range(1, count - 1, 2), range(2, count, 2)) + [(0, 0), (count - 1,) * 2]
        for t in [s ^ 1 if a == b else s]
    ])
    near = lax.ppermute(near, "col", pairs(range(0, count - 1, 2), range(1, count, 2)))
    return near, far


def wide_exchange(parts, slabs, width):
    _, kinds, rows, _ = parts.shape
    tiles = parts.transpose(1, 2, 0, 3).reshape(kinds, rows, slabs, width).transpose(2, 0, 1, 3)
    got = lax.all_to_all(tiles, "slab", 0, 0)
    done = [got[0, what] for what in range(kinds)]
    for s in range(1, slabs):
        done = join(done, [got[s, what] for what in range(kinds)], False)
    return jnp.stack(done)[None]


def swap(x, count, distance):
    low = [i for i in range(count) if not i & distance]
    return lax.ppermute(x, "slab", pairs(low, [i + distance for i in low]))


def body(field, fine_plane, fine_frac, counts):
    slabs = lax.axis_size("slab")
    depth, columns = field.shape[1], field.shape[3]
    width = columns // slabs
    fast = slabs == 4 and width % LANES == 0
    block = width if fast else LANES
    blocks = columns // block

    def block_of(b, s):
        if not fast:
            return b
        parity = jnp.where(b < 2, 1 - (s & 1), s & 1)
        return 2 * (((s >> 1) & 1) ^ 1 ^ (b & 1)) + parity

    follow = lax.ppermute(field[:, :1], "slab", [(i + 1, i) for i in range(slabs - 1)])
    ahead = march(field, fine_plane, fine_frac, counts, block)

    def part(first, steps, coded):
        return close(ahead, follow, depth, first, steps, block_of, coded)

    if not fast:
        parts = part(0, blocks, False)
        image, near, far = finish(wide_exchange(parts, slabs, width), ())
        return border(image, *neighbours(near, far))

    got_a = swap(part(0, 1, True), slabs, 1)
    keep_a = part(2, 1, False)
    got = swap(relay(keep_a, got_a, True), slabs, 2)
    got_b = swap(part(1, 1, True), slabs, 1)
    keep_b = part(3, 1, False)
    image, near, far = finish(relay(keep_b, got_b, False), (got,))
    return border(image, *neighbours(near, far))


def solution(mesh):
    in_specs = (
        P(None, "slab", "col", None),
        P("slab", "col", None),
        P("slab", "col", None),
        P("slab", "col", None),
    )
    out_specs = (P("col", "slab"), P("col", "slab"), P("col", "slab"))

    return jax.shard_map(body, mesh=mesh, in_specs=in_specs, out_specs=out_specs, check_vma=False)
```

```python
import functools

import jax
import jax.numpy as jnp
from jax import lax
from jax.experimental import pallas as pl
from jax.experimental.pallas import tpu as pltpu
from jax.sharding import PartitionSpec as P

LOG2E = 1.4426950408889634
ROWS = 16
LANES = 128
COLOR, DEEP, FINE, COARSE, COARSE_PASS = range(5)
OCTAVES = (22.0, 22.0, 10.0, 22.0, 10.0)
WIRE = jnp.int16


def vmem():
    return pl.BlockSpec(memory_space=pltpu.VMEM)


def encode(x, what):
    y = jnp.maximum(jnp.log2(x) * (65534.0 / OCTAVES[what]) + 65535.5, 0.0)
    return (y.astype(jnp.int32) - 32768).astype(WIRE)


def decode(code, what):
    y = code.astype(jnp.int32).astype(jnp.float32)
    x = jnp.exp2((y - 32767.0) * (OCTAVES[what] / 65534.0))
    return jnp.where(y > -32767.5, x, 0.0)


SCALES = (LOG2E, 0.5)


def shade(raw0, raw1, power):
    soft = jnp.log2(1.0 + jnp.exp2(raw0))
    return jnp.exp2(soft * power), 1.0 + jnp.tanh(raw1)


def march_rows(field, plane, frac, counts, run, late, here, cols, base, total_depth):
    depth, slots = field.shape[1], plane.shape[0]
    unit = 8 if 8 * depth <= 256 else 1
    size = (ROWS, LANES)
    live = counts[0, here, cols]
    color = jnp.zeros(size, jnp.float32)
    deep = jnp.zeros(size, jnp.float32)
    passed = jnp.ones(size, jnp.float32)
    for i in range(slots):
        place = plane[i, here, cols] * 8 + frac[i, here, cols]
        k = (place & 15).astype(jnp.float32)
        to_odd = jnp.minimum(k, 16.0 - k) * 0.125
        place = place.astype(jnp.float32)
        spot = place if unit == 8 else plane[i, here, cols].astype(jnp.float32)
        spot = spot.astype(jnp.bfloat16)
        even = [field[ch, 0, here, cols] for ch in (0, 1)]
        odd = [field[ch, 1, here, cols] for ch in (0, 1)]
        for z in range(1, depth - 1):
            hit = spot >= jnp.bfloat16(unit * z)
            group = even if z % 2 else odd
            for ch in (0, 1):
                group[ch] = jnp.where(hit, field[ch, z + 1, here, cols], group[ch])
        values = []
        for ch in (0, 1):
            e, o = even[ch].astype(jnp.float32), odd[ch].astype(jnp.float32)
            values.append((e + to_odd * (o - e)) * SCALES[ch])
        factor, emission = shade(*values, -(depth / slots) * (2.0 / total_depth))
        rest = jnp.where(live > i, place - 8.0 * (depth - 1), -1.0)
        early = (live > i) & (place < 8.0 * (depth - 1))
        late[i, here, cols] = jnp.maximum(rest, -1.0).astype(jnp.bfloat16)
        factor = jnp.where(early, factor, 1.0)
        weight = passed * (1.0 - factor)
        color = color + weight * emission
        deep = deep + weight * (place + base)
        passed = passed * factor
    run[COLOR, here, cols] = color
    run[DEEP, here, cols] = deep
    run[FINE, here, cols] = passed
    color = jnp.zeros(size, jnp.float32)
    passed = jnp.ones(size, jnp.float32)
    for z in range(7, depth - 1, 8):
        values = [
            (0.5 * SCALES[ch]) * (field[ch, z, here, cols].astype(jnp.float32)
                   + field[ch, z + 1, here, cols].astype(jnp.float32))
            for ch in (0, 1)
        ]
        factor, emission = shade(*values, -8.0 * (2.0 / total_depth))
        color = color + passed * (1.0 - factor) * emission
        passed = passed * factor
    run[COARSE, here, cols] = color
    run[COARSE_PASS, here, cols] = passed


def tiles(rows, width, step):
    across = width // LANES

    def one(at, carry):
        here = pl.ds(pl.multiple_of((at // across) * ROWS, ROWS), ROWS)
        step(here, pl.ds(pl.multiple_of((at % across) * LANES, LANES), LANES))
        return carry

    lax.fori_loop(0, (rows // ROWS) * across, one, 0)


def march(field, plane, frac, counts, slab, steps, block_of, width):
    _, depth, rows, _ = field.shape
    slots = plane.shape[0]
    total_depth = depth * lax.axis_size("slab")

    def kernel(_, field, plane, frac, counts, run, late, last):
        base = (lax.axis_index("slab") * (8 * depth)).astype(jnp.float32)
        last[0] = field[:, depth - 1]
        tiles(rows, width, lambda here, cols: march_rows(
            field, plane, frac, counts, run.at[0], late.at[0], here, cols, base, total_depth
        ))

    def spec(*lead):
        zeros = (0,) * len(lead)
        return pl.BlockSpec(lead + (rows, width), lambda b, s: zeros + (0, block_of(b, s[0])))

    def out(*lead):
        zeros = (0,) * len(lead)
        return pl.BlockSpec((1,) + lead + (rows, width), lambda b, s: (b,) + zeros + (0, 0))

    def shape(*lead, kind):
        return jax.ShapeDtypeStruct((steps,) + lead + (rows, width), kind)

    return pl.pallas_call(
        kernel,
        grid_spec=pltpu.PrefetchScalarGridSpec(
            num_scalar_prefetch=1,
            grid=(steps,),
            in_specs=[spec(2, depth), spec(slots), spec(slots), spec(1)],
            out_specs=[out(5), out(slots), out(2)],
        ),
        out_shape=[
            shape(5, kind=jnp.float32), shape(slots, kind=jnp.bfloat16),
            shape(2, kind=jnp.bfloat16),
        ],
        compiler_params=pltpu.CompilerParams(vmem_limit_bytes=24 << 20),
        cost_estimate=pl.CostEstimate(
            flops=steps * rows * width * 3000, bytes_accessed=steps * rows * width * 128,
            transcendentals=0,
        ),
        name="march",
    )(slab, *(pltpu.with_memory_space_constraint(x, pltpu.HBM)
              for x in (field, plane, frac, counts)))


def close(ahead, follow, depth, steps, run_of, place_of, coded):
    run, late, last = ahead
    _, slots, rows, width = late.shape
    total_depth = depth * lax.axis_size("slab")

    def kernel(run, late, last, follow, out):
        s = lax.axis_index("slab")
        behind = s < lax.axis_size("slab") - 1
        base = (s * (8 * depth) + 8 * (depth - 1)).astype(jnp.float32)

        def step(i, here, cols):
            b = run_of(i, s)
            start = place_of(b, s) * width + cols.start
            there = pl.ds(pl.multiple_of(start, LANES), LANES)
            low = [last[b, ch, here, cols].astype(jnp.float32) * SCALES[ch] for ch in (0, 1)]
            high = [
                jnp.where(behind, follow[ch, 0, here, there].astype(jnp.float32) * SCALES[ch], 0.0)
                for ch in (0, 1)
            ]
            slope = [(h - l) * 0.125 for h, l in zip(high, low)]
            color, deep, passed = (run[b, what, here, cols] for what in (COLOR, DEEP, FINE))
            for k in range(slots):
                eighths = late[b, k, here, cols].astype(jnp.float32)
                values = [l + eighths * d for l, d in zip(low, slope)]
                factor, emission = shade(*values, -(depth / slots) * (2.0 / total_depth))
                factor = jnp.where(eighths >= 0.0, factor, 1.0)
                weight = passed * (1.0 - factor)
                color = color + weight * emission
                deep = deep + weight * (eighths + base)
                passed = passed * factor
            values = [0.5 * (h + l) for h, l in zip(high, low)]
            factor, emission = shade(*values, -8.0 * (2.0 / total_depth))
            coarse, through = (run[b, what, here, cols] for what in (COARSE, COARSE_PASS))
            coarse = coarse + through * (1.0 - factor) * emission
            done = {
                COLOR: 0.5 * color, DEEP: deep * (1.0 / (8.0 * total_depth)), FINE: passed,
                COARSE: 0.5 * coarse, COARSE_PASS: through * factor,
            }
            for what, value in done.items():
                out[i, what, here, cols] = encode(value, what) if coded else value

        for i in range(steps):
            tiles(rows, width, functools.partial(step, i))

    return pl.pallas_call(
        kernel,
        in_specs=[vmem()] * 4,
        out_specs=vmem(),
        out_shape=jax.ShapeDtypeStruct((steps, 5, rows, width), WIRE if coded else jnp.float32),
        compiler_params=pltpu.CompilerParams(vmem_limit_bytes=24 << 20),
        cost_estimate=pl.CostEstimate(
            flops=steps * rows * width * 1500, bytes_accessed=steps * rows * width * 64,
            transcendentals=0,
        ),
        name="close",
    )(run, late, last, follow)


def heads(field, half_of):
    channels, _, rows, columns = field.shape
    width = columns // 2

    def kernel(field, first, second, sem):
        half = half_of(lax.axis_index("slab"))
        copies = [
            pltpu.make_async_copy(
                field.at[ch, 0, :, pl.ds(pl.multiple_of(at * width, width), width)],
                out.at[ch, 0], sem.at[i, ch],
            )
            for i, (out, at) in enumerate(((first, half), (second, 1 - half)))
            for ch in range(channels)
        ]
        for copy in copies:
            copy.start()
        for copy in copies:
            copy.wait()

    return pl.pallas_call(
        kernel,
        in_specs=[pl.BlockSpec(memory_space=pltpu.HBM)],
        out_specs=[vmem()] * 2,
        out_shape=[jax.ShapeDtypeStruct((channels, 1, rows, width), field.dtype)] * 2,
        scratch_shapes=[pltpu.SemaphoreType.DMA((2, channels))],
        compiler_params=pltpu.CompilerParams(vmem_limit_bytes=16 << 20),
        name="heads",
    )(pltpu.with_memory_space_constraint(field, pltpu.HBM))


def join(mine, got, got_first):
    first = [jnp.where(got_first, g, m) for m, g in zip(mine, got)]
    last = [jnp.where(got_first, m, g) for m, g in zip(mine, got)]
    return [
        first[COLOR] + first[FINE] * last[COLOR],
        first[DEEP] + first[FINE] * last[DEEP],
        first[FINE] * last[FINE],
        first[COARSE] + first[COARSE_PASS] * last[COARSE],
        first[COARSE_PASS] * last[COARSE_PASS],
    ]


def relay(mine, got, coded):
    _, kinds, rows, _ = mine.shape

    def kernel(mine, got, send):
        got_first = lax.axis_index("slab") & 1 == 1
        for r in range(0, rows, ROWS):
            here = pl.ds(r, ROWS)
            done = join(
                [mine[0, what, here, :] for what in range(kinds)],
                [decode(got[0, what, here, :], what) for what in range(kinds)],
                got_first,
            )
            for what in range(kinds):
                send[0, what, here, :] = encode(done[what], what) if coded else done[what]

    return pl.pallas_call(
        kernel,
        in_specs=[vmem()] * 2,
        out_specs=vmem(),
        out_shape=jax.ShapeDtypeStruct(got.shape, WIRE if coded else jnp.float32),
        compiler_params=pltpu.CompilerParams(vmem_limit_bytes=16 << 20),
        name="relay",
    )(mine, got)


def finish(mine, got):
    _, kinds, rows, width = mine.shape
    runs = [mine, *got]

    def kernel(mine, *refs):
        *partner, image, near, far = refs
        odd = lax.axis_index("col") % 2 == 1
        done = [mine[0, what] for what in range(kinds)]
        for got in partner:
            got_first = (lax.axis_index("slab") >> 1) & 1 == 1
            done = join(done, [decode(got[0, what], what) for what in range(kinds)], got_first)
        row = lax.broadcasted_iota(jnp.int32, (rows, width), 0)
        for at, what in enumerate((COLOR, DEEP, COARSE)):
            x = done[what]
            up = jnp.where(row == 0, 0.0, pltpu.roll(x, 1, 0))
            down = jnp.where(row == rows - 1, 0.0, pltpu.roll(x, rows - 1, 0))
            image[at] = 0.25 * up + 0.5 * x + 0.25 * down
            top, bottom = x[0:1], x[rows - 1 : rows]
            near[pl.ds(at, 1), :] = 0.25 * jnp.where(odd, top, bottom)
            far[pl.ds(at, 1), :] = 0.25 * jnp.where(odd, bottom, top)

    edge = jax.ShapeDtypeStruct((3, width), jnp.float32)
    return pl.pallas_call(
        kernel,
        in_specs=[vmem()] * len(runs),
        out_specs=[vmem()] * 3,
        out_shape=[jax.ShapeDtypeStruct((3, rows, width), jnp.float32), edge, edge],
        compiler_params=pltpu.CompilerParams(vmem_limit_bytes=16 << 20),
        name="finish",
    )(*runs)


def border(image, near, far):
    _, rows, width = image.shape
    count = lax.axis_size("col")

    def kernel(image, near, far, *outs):
        col = lax.axis_index("col")
        odd = col % 2 == 1
        outermost = (col == 0) | (col == count - 1)
        row = lax.broadcasted_iota(jnp.int32, (rows, width), 0)
        for at, out in enumerate(outs):
            a, b = near[pl.ds(at, 1), :], jnp.where(outermost, 0.0, far[pl.ds(at, 1), :])
            above, below = jnp.where(odd, a, b), jnp.where(odd, b, a)
            extra = jnp.where(row == 0, above, 0.0) + jnp.where(row == rows - 1, below, 0.0)
            out[...] = image[at] + extra

    return pl.pallas_call(
        kernel,
        in_specs=[vmem()] * 3,
        out_specs=[vmem()] * 3,
        out_shape=[jax.ShapeDtypeStruct((rows, width), jnp.float32)] * 3,
        compiler_params=pltpu.CompilerParams(vmem_limit_bytes=16 << 20),
        name="border",
    )(image, near, far)


def pairs(low, high):
    route = list(zip(low, high))
    return route + [(b, a) for a, b in route]


def neighbours(near, far):
    slabs, count = lax.axis_size("slab"), lax.axis_size("col")
    far = lax.ppermute(far, ("slab", "col"), [
        (s * count + a, t * count + b)
        for s in range(slabs)
        for a, b in pairs(range(1, count - 1, 2), range(2, count, 2)) + [(0, 0), (count - 1,) * 2]
        for t in [s ^ 1 if a == b else s]
    ])
    near = lax.ppermute(near, "col", pairs(range(0, count - 1, 2), range(1, count, 2)))
    return near, far


def wide_exchange(parts, slabs, width):
    _, kinds, rows, _ = parts.shape
    tiles = parts.transpose(1, 2, 0, 3).reshape(kinds, rows, slabs, width).transpose(2, 0, 1, 3)
    got = lax.all_to_all(tiles, "slab", 0, 0)
    done = [got[0, what] for what in range(kinds)]
    for s in range(1, slabs):
        done = join(done, [got[s, what] for what in range(kinds)], False)
    return jnp.stack(done)[None]


def swap(x, route):
    return lax.ppermute(x, "slab", route)


def across(count, distance):
    low = [i for i in range(count) if not i & distance]
    return pairs(low, [i + distance for i in low])


def body(field, fine_plane, fine_frac, counts):
    slabs = lax.axis_size("slab")
    depth, columns = field.shape[1], field.shape[3]
    width = columns // slabs
    slab = lax.axis_index("slab").reshape(1).astype(jnp.int32)
    inputs = (field, fine_plane, fine_frac, counts, slab)
    if slabs != 4 or width % LANES:
        blocks = columns // LANES
        ahead = march(*inputs, blocks, lambda b, s: b, LANES)
        follow = lax.ppermute(field[:, :1], "slab", [(i + 1, i) for i in range(slabs - 1)])
        parts = close(ahead, follow, depth, blocks, lambda i, s: i, lambda b, s: b, False)
        image, near, far = finish(wide_exchange(parts, slabs, width), ())
        return border(image, *neighbours(near, far))

    def early(s):
        return 1 - ((s >> 1) & 1)

    ring = [((i + 1) % slabs, i) for i in range(slabs)]
    head_a, head_b = heads(field, lambda s: early((s + slabs - 1) % slabs))
    follow_a = swap(head_a, ring)
    follow_b = swap(head_b, ring)
    theirs, ours = (lambda i, s: 1 - (s & 1)), (lambda i, s: s & 1)

    ahead = march(*inputs, 2, lambda b, s: 2 * early(s) + b, width)
    same = lambda b, s: b
    send_a = close(ahead, follow_a, depth, 1, theirs, same, True)
    got_a = swap(send_a, across(slabs, 1))
    keep_a = close(ahead, follow_a, depth, 1, ours, same, False)
    only = lambda i, s: 0
    ahead = march(*inputs, 1, lambda b, s: 2 * (1 - early(s)) + theirs(b, s), width)
    send_b = close(ahead, follow_b, depth, 1, only, theirs, True)
    got_b = swap(send_b, across(slabs, 1))
    got = swap(relay(keep_a, got_a, True), across(slabs, 2))
    ahead = march(*inputs, 1, lambda b, s: 2 * (1 - early(s)) + ours(b, s), width)
    keep_b = close(ahead, follow_b, depth, 1, only, ours, False)
    image, near, far = finish(relay(keep_b, got_b, False), (got,))
    return border(image, *neighbours(near, far))


def solution(mesh):
    in_specs = (
        P(None, "slab", "col", None),
        P("slab", "col", None),
        P("slab", "col", None),
        P("slab", "col", None),
    )
    out_specs = (P("col", "slab"), P("col", "slab"), P("col", "slab"))

    return jax.shard_map(body, mesh=mesh, in_specs=in_specs, out_specs=out_specs, check_vma=False)
```

```python
import functools

import jax
import jax.numpy as jnp
from jax import lax
from jax.experimental import pallas as pl
from jax.experimental.pallas import tpu as pltpu
from jax.sharding import PartitionSpec as P

LOG2E = 1.4426950408889634
ROWS = 16
LANES = 128
COLOR, DEEP, FINE, COARSE, COARSE_PASS = range(5)
OCTAVES = (22.0, 22.0, 10.0, 22.0, 10.0)
WIRE = jnp.int16


def vmem():
    return pl.BlockSpec(memory_space=pltpu.VMEM)


def encode(x, what):
    y = jnp.maximum(jnp.log2(x) * (65534.0 / OCTAVES[what]) + 65535.5, 0.0)
    return (y.astype(jnp.int32) - 32768).astype(WIRE)


def decode(code, what):
    y = code.astype(jnp.int32).astype(jnp.float32)
    x = jnp.exp2((y - 32767.0) * (OCTAVES[what] / 65534.0))
    return jnp.where(y > -32767.5, x, 0.0)


SCALES = (LOG2E, 0.5)


def shade(raw0, raw1, power):
    soft = jnp.log2(1.0 + jnp.exp2(raw0))
    return jnp.exp2(soft * power), 1.0 + jnp.tanh(raw1)


def march_rows(field, plane, frac, counts, run, late, here, cols, base, total_depth):
    depth, slots = field.shape[1], plane.shape[0]
    unit = 8 if 8 * depth <= 256 else 1
    size = (ROWS, LANES)
    live = counts[0, here, cols]
    color = jnp.zeros(size, jnp.float32)
    deep = jnp.zeros(size, jnp.float32)
    passed = jnp.ones(size, jnp.float32)
    for i in range(slots):
        place = plane[i, here, cols] * 8 + frac[i, here, cols]
        k = (place & 15).astype(jnp.float32)
        to_odd = jnp.minimum(k, 16.0 - k) * 0.125
        place = place.astype(jnp.float32)
        spot = place if unit == 8 else plane[i, here, cols].astype(jnp.float32)
        spot = spot.astype(jnp.bfloat16)
        even = [field[ch, 0, here, cols] for ch in (0, 1)]
        odd = [field[ch, 1, here, cols] for ch in (0, 1)]
        for z in range(1, depth - 1):
            hit = spot >= jnp.bfloat16(unit * z)
            group = even if z % 2 else odd
            for ch in (0, 1):
                group[ch] = jnp.where(hit, field[ch, z + 1, here, cols], group[ch])
        values = []
        for ch in (0, 1):
            e, o = even[ch].astype(jnp.float32), odd[ch].astype(jnp.float32)
            values.append((e + to_odd * (o - e)) * SCALES[ch])
        factor, emission = shade(*values, -(depth / slots) * (2.0 / total_depth))
        rest = jnp.where(live > i, place - 8.0 * (depth - 1), -1.0)
        early = (live > i) & (place < 8.0 * (depth - 1))
        late[i, here, cols] = jnp.maximum(rest, -1.0).astype(jnp.bfloat16)
        factor = jnp.where(early, factor, 1.0)
        weight = passed * (1.0 - factor)
        color = color + weight * emission
        deep = deep + weight * (place + base)
        passed = passed * factor
    run[COLOR, here, cols] = color
    run[DEEP, here, cols] = deep
    run[FINE, here, cols] = passed
    color = jnp.zeros(size, jnp.float32)
    passed = jnp.ones(size, jnp.float32)
    for z in range(7, depth - 1, 8):
        values = [
            (0.5 * SCALES[ch]) * (field[ch, z, here, cols].astype(jnp.float32)
                   + field[ch, z + 1, here, cols].astype(jnp.float32))
            for ch in (0, 1)
        ]
        factor, emission = shade(*values, -8.0 * (2.0 / total_depth))
        color = color + passed * (1.0 - factor) * emission
        passed = passed * factor
    run[COARSE, here, cols] = color
    run[COARSE_PASS, here, cols] = passed


def tiles(rows, width, step):
    across = width // LANES

    def one(at, carry):
        here = pl.ds(pl.multiple_of((at // across) * ROWS, ROWS), ROWS)
        step(here, pl.ds(pl.multiple_of((at % across) * LANES, LANES), LANES))
        return carry

    lax.fori_loop(0, (rows // ROWS) * across, one, 0)


def march(field, plane, frac, counts, width):
    _, depth, rows, columns = field.shape
    slots, steps = plane.shape[0], columns // width
    total_depth = depth * lax.axis_size("slab")

    def kernel(field, plane, frac, counts, run, late, last):
        base = (lax.axis_index("slab") * (8 * depth)).astype(jnp.float32)
        last[0] = field[:, depth - 1]
        tiles(rows, width, lambda here, cols: march_rows(
            field, plane, frac, counts, run.at[0], late.at[0], here, cols, base, total_depth
        ))

    def spec(*lead):
        zeros = (0,) * len(lead)
        return pl.BlockSpec(lead + (rows, width), lambda b: zeros + (0, b))

    def out(*lead):
        zeros = (0,) * len(lead)
        return pl.BlockSpec((1,) + lead + (rows, width), lambda b: (b,) + zeros + (0, 0))

    def shape(*lead, kind):
        return jax.ShapeDtypeStruct((steps,) + lead + (rows, width), kind)

    return pl.pallas_call(
        kernel,
        grid=(steps,),
        in_specs=[spec(2, depth), spec(slots), spec(slots), spec(1)],
        out_specs=[out(5), out(slots), out(2)],
        out_shape=[
            shape(5, kind=jnp.float32), shape(slots, kind=jnp.bfloat16),
            shape(2, kind=jnp.bfloat16),
        ],
        compiler_params=pltpu.CompilerParams(vmem_limit_bytes=24 << 20),
        cost_estimate=pl.CostEstimate(
            flops=steps * rows * width * 3000, bytes_accessed=steps * rows * width * 128,
            transcendentals=0,
        ),
        name="march",
    )(*(pltpu.with_memory_space_constraint(x, pltpu.HBM) for x in (field, plane, frac, counts)))


def close(ahead, follow, depth, first, steps, block_of, coded):
    run, late, last = ahead
    _, slots, rows, width = late.shape
    total_depth = depth * lax.axis_size("slab")

    def kernel(run, late, last, follow, out):
        s = lax.axis_index("slab")
        base = (s * (8 * depth) + 8 * (depth - 1)).astype(jnp.float32)

        def step(i, here, cols):
            b = block_of(first + i, s)
            start = b * width + cols.start
            there = pl.ds(pl.multiple_of(start, LANES), LANES)
            low = [last[b, ch, here, cols].astype(jnp.float32) * SCALES[ch] for ch in (0, 1)]
            high = [follow[ch, 0, here, there].astype(jnp.float32) * SCALES[ch] for ch in (0, 1)]
            slope = [(h - l) * 0.125 for h, l in zip(high, low)]
            color, deep, passed = (run[b, what, here, cols] for what in (COLOR, DEEP, FINE))
            for k in range(slots):
                eighths = late[b, k, here, cols].astype(jnp.float32)
                values = [l + eighths * d for l, d in zip(low, slope)]
                factor, emission = shade(*values, -(depth / slots) * (2.0 / total_depth))
                factor = jnp.where(eighths >= 0.0, factor, 1.0)
                weight = passed * (1.0 - factor)
                color = color + weight * emission
                deep = deep + weight * (eighths + base)
                passed = passed * factor
            values = [0.5 * (h + l) for h, l in zip(high, low)]
            factor, emission = shade(*values, -8.0 * (2.0 / total_depth))
            coarse, through = (run[b, what, here, cols] for what in (COARSE, COARSE_PASS))
            coarse = coarse + through * (1.0 - factor) * emission
            done = {
                COLOR: 0.5 * color, DEEP: deep * (1.0 / (8.0 * total_depth)), FINE: passed,
                COARSE: 0.5 * coarse, COARSE_PASS: through * factor,
            }
            for what, value in done.items():
                out[i, what, here, cols] = encode(value, what) if coded else value

        for i in range(steps):
            tiles(rows, width, functools.partial(step, i))

    return pl.pallas_call(
        kernel,
        in_specs=[vmem()] * 4,
        out_specs=vmem(),
        out_shape=jax.ShapeDtypeStruct((steps, 5, rows, width), WIRE if coded else jnp.float32),
        compiler_params=pltpu.CompilerParams(vmem_limit_bytes=24 << 20),
        cost_estimate=pl.CostEstimate(
            flops=steps * rows * width * 1500, bytes_accessed=steps * rows * width * 64,
            transcendentals=0,
        ),
        name="close",
    )(run, late, last, follow)


def head(field):
    channels, _, rows, columns = field.shape

    def kernel(field, out, sem):
        copies = [
            pltpu.make_async_copy(field.at[ch, 0], out.at[ch, 0], sem.at[ch])
            for ch in range(channels)
        ]
        for copy in copies:
            copy.start()
        for copy in copies:
            copy.wait()

    return pl.pallas_call(
        kernel,
        in_specs=[pl.BlockSpec(memory_space=pltpu.HBM)],
        out_specs=vmem(),
        out_shape=jax.ShapeDtypeStruct((channels, 1, rows, columns), field.dtype),
        scratch_shapes=[pltpu.SemaphoreType.DMA((channels,))],
        compiler_params=pltpu.CompilerParams(vmem_limit_bytes=16 << 20),
        name="head",
    )(pltpu.with_memory_space_constraint(field, pltpu.HBM))


def join(mine, got, got_first):
    first = [jnp.where(got_first, g, m) for m, g in zip(mine, got)]
    last = [jnp.where(got_first, m, g) for m, g in zip(mine, got)]
    return [
        first[COLOR] + first[FINE] * last[COLOR],
        first[DEEP] + first[FINE] * last[DEEP],
        first[FINE] * last[FINE],
        first[COARSE] + first[COARSE_PASS] * last[COARSE],
        first[COARSE_PASS] * last[COARSE_PASS],
    ]


def relay(mine, got, coded):
    _, kinds, rows, _ = mine.shape

    def kernel(mine, got, send):
        got_first = lax.axis_index("slab") & 1 == 1
        for r in range(0, rows, ROWS):
            here = pl.ds(r, ROWS)
            done = join(
                [mine[0, what, here, :] for what in range(kinds)],
                [decode(got[0, what, here, :], what) for what in range(kinds)],
                got_first,
            )
            for what in range(kinds):
                send[0, what, here, :] = encode(done[what], what) if coded else done[what]

    return pl.pallas_call(
        kernel,
        in_specs=[vmem()] * 2,
        out_specs=vmem(),
        out_shape=jax.ShapeDtypeStruct(got.shape, WIRE if coded else jnp.float32),
        compiler_params=pltpu.CompilerParams(vmem_limit_bytes=16 << 20),
        name="relay",
    )(mine, got)


def finish(mine, got):
    _, kinds, rows, width = mine.shape
    runs = [mine, *got]

    def kernel(mine, *refs):
        *partner, image, near, far = refs
        odd = lax.axis_index("col") % 2 == 1
        done = [mine[0, what] for what in range(kinds)]
        for got in partner:
            got_first = (lax.axis_index("slab") >> 1) & 1 == 1
            done = join(done, [decode(got[0, what], what) for what in range(kinds)], got_first)
        row = lax.broadcasted_iota(jnp.int32, (rows, width), 0)
        for at, what in enumerate((COLOR, DEEP, COARSE)):
            x = done[what]
            up = jnp.where(row == 0, 0.0, pltpu.roll(x, 1, 0))
            down = jnp.where(row == rows - 1, 0.0, pltpu.roll(x, rows - 1, 0))
            image[at] = 0.25 * up + 0.5 * x + 0.25 * down
            top, bottom = x[0:1], x[rows - 1 : rows]
            near[pl.ds(at, 1), :] = 0.25 * jnp.where(odd, top, bottom)
            far[pl.ds(at, 1), :] = 0.25 * jnp.where(odd, bottom, top)

    edge = jax.ShapeDtypeStruct((3, width), jnp.float32)
    return pl.pallas_call(
        kernel,
        in_specs=[vmem()] * len(runs),
        out_specs=[vmem()] * 3,
        out_shape=[jax.ShapeDtypeStruct((3, rows, width), jnp.float32), edge, edge],
        compiler_params=pltpu.CompilerParams(vmem_limit_bytes=16 << 20),
        name="finish",
    )(*runs)


def border(image, near, far):
    _, rows, width = image.shape
    count = lax.axis_size("col")

    def kernel(image, near, far, *outs):
        col = lax.axis_index("col")
        odd = col % 2 == 1
        outermost = (col == 0) | (col == count - 1)
        row = lax.broadcasted_iota(jnp.int32, (rows, width), 0)
        for at, out in enumerate(outs):
            a, b = near[pl.ds(at, 1), :], jnp.where(outermost, 0.0, far[pl.ds(at, 1), :])
            above, below = jnp.where(odd, a, b), jnp.where(odd, b, a)
            extra = jnp.where(row == 0, above, 0.0) + jnp.where(row == rows - 1, below, 0.0)
            out[...] = image[at] + extra

    return pl.pallas_call(
        kernel,
        in_specs=[vmem()] * 3,
        out_specs=[vmem()] * 3,
        out_shape=[jax.ShapeDtypeStruct((rows, width), jnp.float32)] * 3,
        compiler_params=pltpu.CompilerParams(vmem_limit_bytes=16 << 20),
        name="border",
    )(image, near, far)


def pairs(low, high):
    route = list(zip(low, high))
    return route + [(b, a) for a, b in route]


def neighbours(near, far):
    slabs, count = lax.axis_size("slab"), lax.axis_size("col")
    far = lax.ppermute(far, ("slab", "col"), [
        (s * count + a, t * count + b)
        for s in range(slabs)
        for a, b in pairs(range(1, count - 1, 2), range(2, count, 2)) + [(0, 0), (count - 1,) * 2]
        for t in [s ^ 1 if a == b else s]
    ])
    near = lax.ppermute(near, "col", pairs(range(0, count - 1, 2), range(1, count, 2)))
    return near, far


def wide_exchange(parts, slabs, width):
    _, kinds, rows, _ = parts.shape
    tiles = parts.transpose(1, 2, 0, 3).reshape(kinds, rows, slabs, width).transpose(2, 0, 1, 3)
    got = lax.all_to_all(tiles, "slab", 0, 0)
    done = [got[0, what] for what in range(kinds)]
    for s in range(1, slabs):
        done = join(done, [got[s, what] for what in range(kinds)], False)
    return jnp.stack(done)[None]


def swap(x, count, distance):
    low = [i for i in range(count) if not i & distance]
    return lax.ppermute(x, "slab", pairs(low, [i + distance for i in low]))


def body(field, fine_plane, fine_frac, counts):
    slabs = lax.axis_size("slab")
    depth, columns = field.shape[1], field.shape[3]
    width = columns // slabs
    fast = slabs == 4 and width % LANES == 0
    block = width if fast else LANES
    blocks = columns // block

    def block_of(b, s):
        if not fast:
            return b
        parity = jnp.where(b < 2, 1 - (s & 1), s & 1)
        return 2 * (((s >> 1) & 1) ^ 1 ^ (b & 1)) + parity

    follow = lax.ppermute(head(field), "slab", [(i + 1, i) for i in range(slabs - 1)])
    ahead = march(field, fine_plane, fine_frac, counts, block)

    def part(first, steps, coded):
        return close(ahead, follow, depth, first, steps, block_of, coded)

    if not fast:
        parts = part(0, blocks, False)
        image, near, far = finish(wide_exchange(parts, slabs, width), ())
        return border(image, *neighbours(near, far))

    got_a = swap(part(0, 1, True), slabs, 1)
    keep_a = part(2, 1, False)
    got = swap(relay(keep_a, got_a, True), slabs, 2)
    got_b = swap(part(1, 1, True), slabs, 1)
    keep_b = part(3, 1, False)
    image, near, far = finish(relay(keep_b, got_b, False), (got,))
    return border(image, *neighbours(near, far))


def solution(mesh):
    in_specs = (
        P(None, "slab", "col", None),
        P("slab", "col", None),
        P("slab", "col", None),
        P("slab", "col", None),
    )
    out_specs = (P("col", "slab"), P("col", "slab"), P("col", "slab"))

    return jax.shard_map(body, mesh=mesh, in_specs=in_specs, out_specs=out_specs, check_vma=False)
```
